256 devices in a mesh: seq: 32 (over x, z), tensor: 8 (over y, core).
Axes of the slice: x: 4, y: 4, z: 8, core: 2. Of those that a mesh axis runs over, the one named last changes fastest.
Arguments:
- hidden_in: bfloat16 [12288, 4096], P('seq', 'tensor'), may hold values from -6 to 6
- norm_gain: float32 [4096], replicated, may hold values from 0.5 to 1.5
- w_x: bfloat16 [4096, 8192], P('seq', 'tensor'), may hold values from -0.09375 to 0.09375
- w_z: bfloat16 [4096, 8192], P('seq', 'tensor'), may hold values from -0.09375 to 0.09375
- w_bc: bfloat16 [4096, 8, 256], P('seq', 'tensor'), may hold values from -0.09375 to 0.09375
- w_dt: bfloat16 [4096, 64], P('seq', 'tensor'), may hold values from -0.09375 to 0.09375
- dt_bias: float32 [64], P('tensor'), may hold values from -6 to -2
- decay_rate: float32 [64], P('tensor'), may hold values from 8.138021e-05 to 8
- conv_x: float32 [4, 8192], P(None, 'tensor'), may hold values from -3 to 3
- conv_bc: float32 [4, 8, 256], P(None, 'tensor'), may hold values from -3 to 3
- conv_bias_x: float32 [8192], P('tensor'), may hold values from -3 to 3
- conv_bias_bc: float32 [8, 256], P('tensor'), may hold values from -3 to 3
- skip_d: float32 [64], P('tensor'), may hold values from 0.5 to 8
- out_gain: float32 [8192], P('tensor'), may hold values from 0.5 to 1.5
- w_out: bfloat16 [8192, 4096], P('tensor'), may hold values from -0.0625 to 0.0625
Outputs:
- layer_out: bfloat16 [12288, 4096], P('seq', 'tensor')
The draws below stay inside these ranges and needn't reach their ends.
All inputs are finite; a program needn't handle non-finite values.
Results may differ from the reference program's by a relative error of at most 0.0095.
Values may be sent and summed in bfloat16 or wider, within the bound.
No kernel may reach another device: no remote copies, remote signals or barrier semaphores. Data moves between devices by JAX's collectives and lax.ppermute only.
A program may use at most 128 MiB of HBM per device.

```python
import math
import jax
import jax.numpy as jnp
from jax import lax

D = 4096
H = 64
P_SIZE = 128
N = 128
G = 8
KCONV = 4
SPAN = 128
DI = 8192
TOKENS = 12288


def shard_levels(stream_key, extent, cuts, smallest, largest):
    loudness, own = 1.0, jax.random.fold_in(stream_key, 6)
    for position, shards_of in cuts:
        draws = jnp.exp(jax.random.uniform(jax.random.fold_in(own, position), (shards_of,), jnp.float32, smallest / len(cuts), largest / len(cuts)))
        loudness = loudness * jnp.repeat(draws, extent[position] // shards_of).reshape([-1 if axis == position else 1 for axis in range(len(extent))])
    return loudness


def centred(stream_key, shape, deviation, most, split=(), dtype=jnp.bfloat16):
    gain = shard_levels(stream_key, shape, split, -0.22, 0.18) if split else 1.0
    entries = jax.random.normal(stream_key, shape, jnp.float32) * deviation * gain
    return jnp.minimum(jnp.maximum(entries, -most), most).astype(dtype)


def setup_inputs(seed: int = 0) -> dict:
    seeds = jax.random.split(jax.random.key(seed), 16)
    hidden_in = centred(seeds[0], (TOKENS, D), 1.0, 6.0, ((0, 32), (1, 8)))
    norm_gain = jnp.clip(1.0 + 0.1 * jax.random.normal(seeds[1], (D,), jnp.float32), 0.5, 1.5)
    w_x = centred(seeds[2], (D, DI), D ** -0.5, 0.09375, ((0, 32), (1, 8)))
    w_z = centred(seeds[3], (D, DI), D ** -0.5, 0.09375, ((0, 32), (1, 8)))
    w_bc = centred(seeds[4], (D, G, 2 * N), D ** -0.5, 0.09375, ((0, 32), (1, 8)))
    w_dt = centred(seeds[5], (D, H), D ** -0.5, 0.09375, ((0, 32), (1, 8)))
    dt_bias = jnp.clip(-6.0 + 4.0 * jax.random.uniform(seeds[6], (H,), jnp.float32) ** shard_levels(seeds[6], (H,), ((0, 8),), -0.2, 0.2), -6.0, -2.0)
    decay_rate = jnp.clip(jnp.exp(math.log(8.0) - 11.49582 * jax.random.uniform(seeds[7], (H,), jnp.float32) ** shard_levels(seeds[7], (H,), ((0, 8),), -0.2, 0.2)), 8.138021075865254e-05, 8.0)
    conv_x = centred(seeds[8], (KCONV, DI), KCONV ** -0.5, 3.0, ((1, 8),), jnp.float32)
    conv_bc = centred(seeds[9], (KCONV, G, 2 * N), KCONV ** -0.5, 3.0, ((1, 8),), jnp.float32)
    conv_bias_x = centred(seeds[10], (DI,), 0.5, 3.0, ((0, 8),), jnp.float32)
    conv_bias_bc = centred(seeds[11], (G, 2 * N), 0.5, 3.0, ((0, 8),), jnp.float32)
    skip_d = jnp.clip(jnp.exp(math.log(8.0) - 2.7725887 * jax.random.uniform(seeds[12], (H,), jnp.float32) ** shard_levels(seeds[12], (H,), ((0, 8),), -0.2, 0.2)), 0.5, 8.0)
    out_gain = jnp.clip(1.0 + 0.1 * jax.random.normal(seeds[13], (DI,), jnp.float32), 0.5, 1.5)
    w_out = centred(seeds[14], (DI, D), DI ** -0.5, 0.0625, ((0, 8),))
    return {"hidden_in": hidden_in, "norm_gain": norm_gain, "w_x": w_x, "w_z": w_z, "w_bc": w_bc, "w_dt": w_dt, "dt_bias": dt_bias, "decay_rate": decay_rate, "conv_x": conv_x, "conv_bc": conv_bc, "conv_bias_x": conv_bias_x, "conv_bias_bc": conv_bias_bc, "skip_d": skip_d, "out_gain": out_gain, "w_out": w_out}


epsilon = 1e-05

def rms_scale(values, norm_weight):
    return values * lax.rsqrt(lax.optimization_barrier(jnp.mean(values * values, axis=-1, keepdims=True)) + epsilon) * norm_weight

def causal_conv(padded, weight, bias_row):
    tap_count = weight.shape[0]
    out_length = padded.shape[0] - tap_count + 1
    running = bias_row.astype(jnp.float32)
    for k in range(tap_count):
        running = running + weight[k].astype(jnp.float32) * padded[k:k + out_length].astype(jnp.float32)
    return jax.nn.silu(running).astype(jnp.bfloat16)

def span_terms(x_blocks, b_blocks, c_blocks, log_decay, dt_blocks):
    cum_decay = jnp.cumsum(log_decay, axis=1)
    scores = jnp.einsum('ctgn,csgn->cgts', c_blocks.astype(jnp.float32), b_blocks.astype(jnp.float32))
    length = x_blocks.shape[1]
    causal_mask = lax.broadcasted_iota(jnp.int32, (length, length), 0) >= lax.broadcasted_iota(jnp.int32, (length, length), 1)
    cum_rows = jnp.transpose(cum_decay, (0, 2, 3, 1))
    decay_gap = cum_rows[..., :, None] - cum_rows[..., None, :]
    decay_mat = jnp.where(causal_mask, jnp.exp(jnp.where(causal_mask, decay_gap, 0.0)), 0.0)
    dt_cols = jnp.transpose(dt_blocks, (0, 2, 3, 1))[..., None, :]
    mix_weight = (scores[:, :, None] * decay_mat * dt_cols).astype(jnp.bfloat16)
    intra_out = jnp.einsum('cgkts,csgkp->ctgkp', mix_weight.astype(jnp.float32), x_blocks.astype(jnp.float32))
    tail_decay = jnp.exp(cum_decay[:, -1:] - cum_decay) * dt_blocks
    scaled = (x_blocks.astype(jnp.float32) * tail_decay[..., None]).astype(jnp.bfloat16)
    fresh_state = jnp.einsum('csgkp,csgn->cgkpn', scaled.astype(jnp.float32), b_blocks.astype(jnp.float32))
    return (cum_decay, intra_out, fresh_state)

def reference(hidden_in, norm_gain, w_x, w_z, w_bc, w_dt, dt_bias, decay_rate, conv_x, conv_bc, conv_bias_x, conv_bias_bc, skip_d, out_gain, w_out):
    per_group = H // G
    span_count = TOKENS // SPAN
    rim_rows = KCONV - 1
    normed = rms_scale(hidden_in.astype(jnp.float32), norm_gain).astype(jnp.bfloat16)
    proj_x = jnp.dot(normed, w_x, preferred_element_type=jnp.float32).astype(jnp.bfloat16)
    gate_z = jnp.dot(normed, w_z, preferred_element_type=jnp.float32).astype(jnp.bfloat16)
    proj_bc = jnp.dot(normed, w_bc.reshape(D, G * 2 * N), preferred_element_type=jnp.float32).astype(jnp.bfloat16).reshape(TOKENS, G, 2 * N)
    dt_vals = jax.nn.softplus(jnp.dot(normed, w_dt, preferred_element_type=jnp.float32) + dt_bias)
    x_conv = causal_conv(jnp.concatenate([jnp.zeros((rim_rows, DI), jnp.bfloat16), proj_x], axis=0), conv_x, conv_bias_x)
    bc_conv = causal_conv(jnp.concatenate([jnp.zeros((rim_rows, G, 2 * N), jnp.bfloat16), proj_bc], axis=0), conv_bc, conv_bias_bc)
    x_blocks = x_conv.reshape(span_count, SPAN, G, per_group, P_SIZE)
    b_blocks = bc_conv[..., :N].reshape(span_count, SPAN, G, N)
    c_blocks = bc_conv[..., N:].reshape(span_count, SPAN, G, N)
    log_decay = (-dt_vals * decay_rate).reshape(span_count, SPAN, G, per_group)
    dt_blocks = dt_vals.reshape(span_count, SPAN, G, per_group)
    skip_heads = skip_d.reshape(G, per_group)[..., None]

    def span_step(state_in, block_item):
        x_block, b_block, c_block, log_block, dt_block = [piece[None] for piece in block_item]
        cum_decay, intra_out, fresh_state = span_terms(x_block, b_block, c_block, log_block, dt_block)
        inter_out = jnp.exp(cum_decay)[..., None] * jnp.einsum('ctgn,gkpn->ctgkp', c_block.astype(jnp.float32), state_in, precision=lax.Precision.HIGHEST)
        ssm_out = intra_out + inter_out + skip_heads * x_block.astype(jnp.float32)
        state_next = jnp.exp(cum_decay[0, -1])[..., None, None] * state_in + fresh_state[0]
        return (state_next, ssm_out[0])
    start_state = jnp.zeros((G, per_group, P_SIZE, N), jnp.float32)
    final_state, ssm_out = lax.scan(span_step, start_state, (x_blocks, b_blocks, c_blocks, log_decay, dt_blocks))
    ssm_out = ssm_out.reshape(TOKENS, DI)
    gated_out = ssm_out * jax.nn.silu(gate_z.astype(jnp.float32))
    grouped = gated_out.reshape(TOKENS, G, DI // G)
    normed_y = rms_scale(grouped, out_gain.reshape(G, DI // G)).reshape(TOKENS, DI).astype(jnp.bfloat16)
    mixed = jnp.dot(normed_y, w_out, preferred_element_type=jnp.float32)
    return (hidden_in.astype(jnp.float32) + mixed).astype(jnp.bfloat16)
```

```python
import functools

import jax
import jax.numpy as jnp
from jax import lax
from jax.experimental import pallas as pl
from jax.experimental.pallas import tpu as pltpu
from jax.sharding import Mesh
from jax.sharding import PartitionSpec as P

SPAN = 128
LEAD = 16
EPS = 1e-05
F32, BF16 = jnp.float32, jnp.bfloat16


def dot(a, b):
    return jnp.dot(a, b, preferred_element_type=F32)


def shifted(block, axis, distance):
    n = lax.axis_size(axis)
    return lax.ppermute(block, axis, [(i, (i + distance) % n) for i in range(n)])


def silu(v):
    return v * jax.nn.sigmoid(v)


def proj_kernel(h_ref, w_ref, taps_ref, bias_ref, dt_bias_ref, x_ref, bc_ref, dt_ref, z_ref, acc, pre):
    pieces, feats = h_ref.shape[1], h_ref.shape[3]
    part, total, low = x_ref.shape[2], pieces * feats, pre.shape[1]
    rows = x_ref.shape[1]
    squares = jnp.zeros((h_ref.shape[2], 1), F32)
    for j in range(pieces):
        h = h_ref[0, j]
        product = dot(h, w_ref[j * feats : (j + 1) * feats, :])
        if j == 0:
            acc[...] = product
        else:
            acc[...] += product
        wide = h.astype(F32)
        squares = squares + jnp.sum(wide * wide, axis=1, keepdims=True)
    scale = lax.rsqrt(squares / total + EPS)
    z_ref[0] = (acc[LEAD:, low:] * scale[LEAD:]).astype(BF16)
    pre[...] = acc[:, :low] * scale
    dt_raw = pre[LEAD:, part:] + dt_bias_ref[...]
    dt_ref[0] = jnp.maximum(dt_raw, 0.0) + jnp.log1p(jnp.exp(-jnp.abs(dt_raw)))
    pre[...] = pre[...].astype(BF16).astype(F32)
    taps = taps_ref.shape[0]
    running = bias_ref[...]
    for k in range(taps):
        start = LEAD - taps + 1 + k
        running = running + taps_ref[k : k + 1] * pre[start : start + rows]
    mixed = silu(running).astype(BF16)
    x_ref[0] = mixed[:, :part]
    bc_ref[0] = mixed[:, part:]


def project(h, w, taps, bias, dt_bias, part):
    segments, pieces, tall, feats = h.shape
    rows, lanes, low = tall - LEAD, w.shape[1], taps.shape[1]
    whole = lambda a: pl.BlockSpec(a.shape, lambda s: (0,) * a.ndim)
    out = lambda width: pl.BlockSpec((1, rows, width), lambda s: (s, 0, 0))
    shape = lambda width, dtype: jax.ShapeDtypeStruct((segments, rows, width), dtype)
    return pl.pallas_call(
        proj_kernel,
        grid=(segments,),
        in_specs=[
            pl.BlockSpec((1, pieces, tall, feats), lambda s: (s, 0, 0, 0)),
            whole(w),
            whole(taps),
            whole(bias),
            whole(dt_bias),
        ],
        out_specs=[out(part), out(low - part), out(low - part), out(lanes - low)],
        out_shape=[
            shape(part, BF16),
            shape(low - part, BF16),
            shape(low - part, F32),
            shape(lanes - low, BF16),
        ],
        scratch_shapes=[pltpu.VMEM((tall, lanes), F32), pltpu.VMEM((tall, low), F32)],
        name="project",
    )(h, w, taps, bias, dt_bias)


def scan_kernel(first, head, x_ref, b_ref, c_ref, dt_ref, rate_ref, skip_ref, y_ref, cum_ref, s_ref, total_ref):
    rows, part = x_ref.shape[1:]
    heads = part // head
    n = b_ref.shape[2]
    pick = lambda axis: lax.broadcasted_iota(jnp.int32, (SPAN, SPAN), axis)
    mask = pick(0) >= pick(1)
    lower = mask.astype(F32)
    base = jnp.zeros_like(rate_ref[...])
    states = [None] * heads
    for b in range(rows // SPAN):
        at = slice(b * SPAN, (b + 1) * SPAN)
        dt = dt_ref[0, at]
        cum = jnp.dot(
            lower, -dt * rate_ref[...], precision=lax.Precision.HIGHEST, preferred_element_type=F32
        )
        cum_rows, dt_rows = cum.T, dt.T
        b_block, c_block = b_ref[0, at], c_ref[0, at]
        scores = lax.dot_general(
            c_block, b_block, (((1,), (1,)), ((), ())), preferred_element_type=F32
        )
        b_cols = b_block.T
        last = cum[SPAN - 1 : SPAN]
        tail = jnp.exp(last - cum) * dt
        for h in range(heads):
            lane = slice(first + h, first + h + 1)
            cols = slice(h * head, (h + 1) * head)
            gap = cum[:, lane] - cum_rows[lane]
            decay = jnp.where(mask, jnp.exp(jnp.where(mask, gap, 0.0)), 0.0)
            mix = (scores * decay * dt_rows[lane]).astype(BF16)
            x = x_ref[0, at, cols]
            wide = x.astype(F32)
            y = dot(mix, x) + skip_ref[:, cols] * wide
            fresh = dot(b_cols, (wide * tail[:, lane]).astype(BF16))
            if b:
                y = y + jnp.exp(cum[:, lane]) * dot(c_block, states[h].astype(BF16))
                fresh = jnp.exp(last[:, lane]) * states[h] + fresh
            states[h] = fresh
            y_ref[0, at, cols] = y
        cum_ref[0, at] = cum + base
        base = base + last
    chunks = s_ref.shape[0]
    for h in range(heads):
        cols = slice(h * head, (h + 1) * head)
        s_ref[:, 0, :, cols] = states[h].reshape(chunks, n // chunks, head).astype(BF16)
        total_ref[0, :, cols] = jnp.broadcast_to(
            base[:, first + h : first + h + 1], (total_ref.shape[1], head)
        )


def scan_blocks(x, b, c, dt, rate, skip, first, head, chunks):
    segments, rows, part = x.shape
    n = b.shape[2]
    each = lambda a: pl.BlockSpec((1, *a.shape[1:]), lambda s: (s, 0, 0))
    whole = lambda a: pl.BlockSpec(a.shape, lambda s: (0,) * a.ndim)
    return pl.pallas_call(
        functools.partial(scan_kernel, first, head),
        grid=(segments,),
        in_specs=[each(x), each(b), each(c), each(dt), whole(rate), whole(skip)],
        out_specs=[
            each(x),
            each(dt),
            pl.BlockSpec((chunks, 1, n // chunks, part), lambda s: (0, s, 0, 0)),
            pl.BlockSpec((1, 8, part), lambda s: (s, 0, 0)),
        ],
        out_shape=[
            jax.ShapeDtypeStruct(x.shape, F32),
            jax.ShapeDtypeStruct(dt.shape, F32),
            jax.ShapeDtypeStruct((chunks, segments, n // chunks, part), BF16),
            jax.ShapeDtypeStruct((segments, 8, part), F32),
        ],
        name="scan_blocks",
    )(x, b, c, dt, rate, skip)


def combine_kernel(segments, r_ref, o_ref):
    places, part = r_ref.shape[0], r_ref.shape[2]
    deep = o_ref.shape[1] // segments
    logs = r_ref[:, segments * deep :, :].astype(F32)
    state = jnp.zeros((deep, part), F32)
    for s in range(segments):
        at = slice(s * deep, (s + 1) * deep)
        for z in range(places):
            o_ref[z, at] = state.astype(BF16)
            decay = jnp.exp(logs[z, 2 * s : 2 * s + 1] + logs[z, 2 * s + 1 : 2 * s + 2])
            state = decay * state + r_ref[z, at].astype(F32)


def combine_states(received, segments):
    places, deep, part = received.shape
    return pl.pallas_call(
        functools.partial(combine_kernel, segments),
        out_shape=jax.ShapeDtypeStruct((places, deep - 2 * segments, part), BF16),
        name="combine_states",
    )(received)


def gate_kernel(first, head, y_ref, cum_ref, c_ref, s_ref, z_ref, o_ref):
    part = y_ref.shape[2]
    enter = s_ref[...].reshape(c_ref.shape[2], part)
    inter = dot(c_ref[0], enter)
    for h in range(part // head):
        cols = slice(h * head, (h + 1) * head)
        grow = jnp.exp(cum_ref[0, :, first + h : first + h + 1])
        y = y_ref[0, :, cols] + grow * inter[:, cols]
        o_ref[0, :, cols] = (y * silu(z_ref[0, :, cols].astype(F32))).astype(BF16)


def gate_blocks(y, cum, c, entering, z, first, head):
    segments, rows, part = y.shape
    deep = entering.shape[1] // segments
    each = lambda a: pl.BlockSpec((1, *a.shape[1:]), lambda s: (s, 0, 0))
    return pl.pallas_call(
        functools.partial(gate_kernel, first, head),
        grid=(segments,),
        in_specs=[
            each(y),
            each(cum),
            each(c),
            pl.BlockSpec((entering.shape[0], deep, part), lambda s: (0, s, 0)),
            each(z),
        ],
        out_specs=each(z),
        out_shape=jax.ShapeDtypeStruct(z.shape, BF16),
        name="gate_blocks",
    )(y, cum, c, entering, z)


def out_kernel(side_ref, g_ref, gain_ref, w_ref, o_ref, normed):
    quarters, rows, part = g_ref.shape

    @pl.when(pl.program_id(0) == 0)
    def _():
        squares = jnp.zeros((rows, 1), F32)
        for q in range(quarters):
            g = g_ref[q].astype(F32)
            squares = squares + jnp.sum(g * g, axis=1, keepdims=True)
        scale = lax.rsqrt(squares / (quarters * part) + EPS)
        for q in range(quarters):
            cols = slice(q * part, (q + 1) * part)
            normed[:, cols] = (g_ref[q].astype(F32) * scale * gain_ref[:, cols]).astype(BF16)

    o_ref[0] = dot(normed[...], w_ref[...]).astype(BF16)


def out_partial(side, g, gain, w, places, sides):
    quarters, rows, part = g.shape
    width = w.shape[1] // (places * sides)
    return pl.pallas_call(
        out_kernel,
        grid_spec=pltpu.PrefetchScalarGridSpec(
            num_scalar_prefetch=1,
            grid=(places,),
            in_specs=[
                pl.BlockSpec(g.shape, lambda i, s: (0, 0, 0)),
                pl.BlockSpec(gain.shape, lambda i, s: (0, 0)),
                pl.BlockSpec((w.shape[0], width), lambda i, s: (0, i * sides + s[0])),
            ],
            out_specs=pl.BlockSpec((1, rows, width), lambda i, s: (i, 0, 0)),
            scratch_shapes=[pltpu.VMEM((rows, quarters * part), BF16)],
        ),
        out_shape=jax.ShapeDtypeStruct((places, rows, width), BF16),
        name="out_partial",
    )(jnp.full((1,), side, jnp.int32), g, gain, w)


def gathered_weights(packed, low):
    nz, zi = lax.axis_size("z"), lax.axis_index("z")
    segments, depth, lanes = packed.shape
    whole = jnp.zeros((segments, nz, depth, lanes), BF16)

    def placed(whole, block, distance, lane):
        place = lax.rem(zi + distance + nz, nz)
        return lax.dynamic_update_slice(whole, block[:, None], (0, place, 0, lane))

    whole = placed(whole, packed, 0, 0)
    left = right = packed
    for step in range(1, nz // 2):
        left, right = shifted(left, "z", 1), shifted(right, "z", -1)
        whole = placed(placed(whole, left, -step, 0), right, step, 0)
    half = nz // 2
    left, right = shifted(left[..., :low], "z", 1), shifted(right[..., low:], "z", -1)
    whole = placed(placed(whole, left, -half, 0), right, half, low)
    return whole.reshape(segments * nz * depth, lanes)


def local(
    hidden_in,
    norm_gain,
    w_x,
    w_z,
    w_bc,
    w_dt,
    dt_bias,
    decay_rate,
    conv_x,
    conv_bc,
    conv_bias_x,
    conv_bias_bc,
    skip_d,
    out_gain,
    w_out,
):
    nx, nz, ny, nc = (lax.axis_size(a) for a in ("x", "z", "y", "c"))
    xi, zi, ci = (lax.axis_index(a) for a in ("x", "z", "c"))
    rows, feats = hidden_in.shape
    depth, width = w_x.shape
    part = width // nx
    bc_width = w_bc.shape[2]
    bc_part = bc_width // nx
    heads = decay_rate.shape[0]
    own_heads = heads // nx
    taps = conv_x.shape[0]
    low = -(-(part + bc_part + own_heads) // 128) * 128
    spare = low - part - bc_part - own_heads

    route = [(i, i + 1) for i in range(nx * nz - 1)]
    edge = lax.ppermute(hidden_in[rows - LEAD :], ("x", "z"), route)
    tall = jnp.concatenate([edge, hidden_in], axis=0)
    gathered = lax.all_gather(tall, ("x", "y", "c"), axis=0)
    gathered = gathered.reshape(nx, ny * nc, rows + LEAD, feats)

    gain = lax.dynamic_slice(norm_gain, ((xi * nz + zi) * depth,), (depth,))
    pieces = [w.reshape(depth, nx, -1) for w in (w_x, w_bc, w_dt)]
    pieces.append(jnp.zeros((depth, nx, spare), BF16))
    pieces.append(w_z.reshape(depth, nx, part))
    packed = jnp.concatenate(pieces, axis=2).astype(F32) * gain[:, None, None]
    packed = jnp.transpose(packed.astype(BF16), (1, 0, 2))
    packed = lax.all_to_all(packed, "x", 0, 0, tiled=True)
    weights = gathered_weights(packed, low)

    def own(a):
        size = a.shape[-1] // nx
        return lax.dynamic_slice_in_dim(a, xi * size, size, axis=a.ndim - 1)

    row = lambda a: a.reshape(1, -1)
    tap_rows = jnp.concatenate([own(conv_x), own(conv_bc.reshape(taps, -1))], axis=1)
    tap_rows = jnp.pad(tap_rows, ((0, 0), (0, own_heads + spare)))
    bias_row = jnp.concatenate([own(conv_bias_x), own(conv_bias_bc.reshape(-1))])
    bias_row = row(jnp.pad(bias_row, (0, own_heads + spare)))
    in_lanes = lambda a: row(jnp.pad(own(a), (bc_part, spare)))
    x_conv, bc_conv, dt, gate_z = project(
        gathered, weights, tap_rows, bias_row, in_lanes(dt_bias), part
    )

    half = nx // 2
    quarter = bc_conv[:, :, :bc_part]
    quarter = jnp.concatenate([quarter[:half], quarter[half:]], axis=2)
    quarters = lax.all_to_all(
        jnp.broadcast_to(quarter[None], (nx, *quarter.shape)), "x", 0, 0, tiled=True
    )
    both = jnp.concatenate([quarters[..., :bc_part], quarters[..., bc_part:]], axis=1)
    b_rows = jnp.concatenate([both[q] for q in range(half)], axis=2)
    c_rows = jnp.concatenate([both[q] for q in range(half, nx)], axis=2)

    skip_row = row(jnp.repeat(own(skip_d), width // heads))
    y, cum, states, totals = scan_blocks(
        x_conv, b_rows, c_rows, dt, in_lanes(decay_rate), skip_row, bc_part, width // heads, nz
    )
    logs = totals[:, 0]
    high = logs.astype(BF16)
    logs = jnp.stack([high, (logs - high.astype(F32)).astype(BF16)], axis=1)
    logs = jnp.broadcast_to(logs.reshape(1, 2 * nx, part), (nz, 2 * nx, part))
    message = jnp.concatenate([states.reshape(nz, -1, part), logs], axis=1)
    received = lax.all_to_all(message, "z", 0, 0, tiled=True)
    entering = lax.all_to_all(combine_states(received, nx), "z", 0, 0, tiled=True)
    gated = gate_blocks(y, cum, c_rows, entering, gate_z, bc_part, width // heads)
    gated = lax.all_to_all(gated, "x", 0, 0, tiled=True)

    gain_row = row(out_gain)
    theirs = out_partial(1 - ci, gated, gain_row, w_out, ny, nc)
    theirs = shifted(theirs, "c", 1)
    ours = out_partial(ci, gated, gain_row, w_out, ny, nc)
    ours = (ours.astype(F32) + theirs.astype(F32)).astype(BF16)
    shares = lax.all_to_all(ours, "y", 0, 0, tiled=True)
    summed = jnp.sum(shares.astype(F32), axis=0)
    return (hidden_in.astype(F32) + summed).astype(BF16)


def solution(mesh):
    sizes = mesh.shape
    devices = mesh.devices.reshape(4, sizes["seq"] // 4, sizes["tensor"] // 2, 2)
    split = Mesh(devices, ("x", "z", "y", "c"))
    seq, tensor = ("x", "z"), ("y", "c")
    in_specs = (
        P(seq, tensor),
        P(),
        P(seq, tensor),
        P(seq, tensor),
        P(seq, tensor, None),
        P(seq, tensor),
        P(tensor),
        P(tensor),
        P(None, tensor),
        P(None, tensor, None),
        P(tensor),
        P(tensor, None),
        P(tensor),
        P(tensor),
        P(tensor, None),
    )
    return jax.shard_map(
        local, mesh=split, in_specs=in_specs, out_specs=P(seq, tensor), check_vma=False
    )
```

```python
import functools

import jax
import jax.numpy as jnp
from jax import lax
from jax.experimental import pallas as pl
from jax.experimental.pallas import tpu as pltpu
from jax.sharding import Mesh
from jax.sharding import PartitionSpec as P

SPAN = 128
LEAD = 16
EPS = 1e-05
F32, BF16 = jnp.float32, jnp.bfloat16


def dot(a, b):
    return jnp.dot(a, b, preferred_element_type=F32)


def shifted(block, axis, distance):
    n = lax.axis_size(axis)
    return lax.ppermute(block, axis, [(i, (i + distance) % n) for i in range(n)])


def silu(v):
    return v * jax.nn.sigmoid(v)


def whole(a):
    return pl.BlockSpec(a.shape, lambda s: (0,) * a.ndim)


def each(a):
    return pl.BlockSpec((1, *a.shape[1:]), lambda s: (s,) + (0,) * (a.ndim - 1))


def cost(flops, *arrays):
    moved = sum(a.size * a.dtype.itemsize for a in arrays)
    return pl.CostEstimate(flops=flops, bytes_accessed=moved, transcendentals=0)


def proj_kernel(halves, edge_ref, h_ref, w_ref, taps_ref, bias_ref, dt_bias_ref, x_ref, bc_ref, dt_ref, acc, pre):
    pieces, feats = h_ref.shape[1], h_ref.shape[3]
    part, total = x_ref.shape[2], pieces * feats
    rows, bc_part = x_ref.shape[1], bc_ref.shape[3] // halves
    lanes = min(128, feats)
    step = pieces // 2
    squares = None
    for j in range(0, pieces, step):
        tall = []
        for i in range(j, j + step):
            h = jnp.concatenate([edge_ref[0, i], h_ref[0, i]], axis=0)
            tall.append(h)
            wide = h.astype(F32)
            for k in range(0, feats, lanes):
                square = wide[:, k : k + lanes] * wide[:, k : k + lanes]
                squares = square if squares is None else squares + square
        product = dot(jnp.concatenate(tall, axis=1), w_ref[j * feats : (j + step) * feats, :])
        if j == 0:
            acc[...] = product
        else:
            acc[...] += product
    scale = lax.rsqrt(jnp.sum(squares, axis=1, keepdims=True) / total + EPS)
    spare = dt_ref.shape[2]
    dt_raw = acc[LEAD:, part:] * scale[LEAD:] + dt_bias_ref[...]
    dt = jnp.maximum(dt_raw, 0.0) + jnp.log1p(jnp.exp(-jnp.abs(dt_raw)))
    lane = lax.broadcasted_iota(jnp.int32, dt.shape, 1)
    dt_ref[0] = jnp.where(lane == spare - 1, scale[LEAD:], dt)
    pre[...] = (acc[...] * scale).astype(BF16).astype(F32)
    taps = taps_ref.shape[0]
    running = bias_ref[...]
    for k in range(taps):
        start = LEAD - taps + 1 + k
        running = running + taps_ref[k : k + 1] * pre[start : start + rows]
    mixed = silu(running).astype(BF16)
    x_ref[0] = mixed[:, :part]
    quarter = mixed[:, part : part + bc_part]
    for side in range(halves):

        @pl.when(lax.rem(pl.program_id(0), halves) == side)
        def _():
            for q in range(bc_ref.shape[0]):
                bc_ref[q, 0, :, side * bc_part : (side + 1) * bc_part] = quarter


def project(edge, h, w, taps, bias, dt_bias, part, bc_part):
    segments, pieces, rows, feats = h.shape
    low = w.shape[1]
    out = lambda width: pl.BlockSpec((1, rows, width), lambda s: (s, 0, 0))
    shape = lambda width, dtype: jax.ShapeDtypeStruct((segments, rows, width), dtype)
    packed = (segments, segments // 2, rows, 2 * bc_part)
    return pl.pallas_call(
        functools.partial(proj_kernel, 2),
        grid=(segments,),
        in_specs=[each(edge), each(h), whole(w), whole(taps), whole(bias), whole(dt_bias)],
        out_specs=[
            out(part),
            pl.BlockSpec((segments, 1, *packed[2:]), lambda s: (0, s // 2, 0, 0)),
            out(low - part),
        ],
        out_shape=[
            shape(part, BF16),
            jax.ShapeDtypeStruct(packed, BF16),
            shape(low - part, F32),
        ],
        scratch_shapes=[pltpu.VMEM((rows + LEAD, low), F32), pltpu.VMEM((rows + LEAD, low), F32)],
        cost_estimate=cost(2 * h.size * low, h, w),
        name="project",
    )(edge, h, w, taps, bias, dt_bias)


def gate_proj_kernel(h_ref, w_ref, dt_ref, z_ref):
    pieces = h_ref.shape[1]
    tall = jnp.concatenate([h_ref[0, j] for j in range(pieces)], axis=1)
    scale = dt_ref[0, :, dt_ref.shape[2] - 1 :]
    z_ref[0] = (dot(tall, w_ref[...]) * scale).astype(BF16)


def project_gate(h, w, dt):
    segments, pieces, rows, feats = h.shape
    part = w.shape[1]
    return pl.pallas_call(
        gate_proj_kernel,
        grid=(segments,),
        in_specs=[each(h), whole(w), each(dt)],
        out_specs=pl.BlockSpec((1, rows, part), lambda s: (s, 0, 0)),
        out_shape=jax.ShapeDtypeStruct((segments, rows, part), BF16),
        cost_estimate=cost(2 * h.size * part, h, w),
        name="project_gate",
    )(h, w, dt)


def group_rows(quarters_ref, at, first):
    count, width = quarters_ref.shape[0] // 2, quarters_ref.shape[3] // 2
    odd = lax.rem(pl.program_id(0), 2) == 1
    parts = []
    for q in range(count):
        pair = quarters_ref[first * count + q, 0, at]
        parts.append(jnp.where(odd, pair[:, width:], pair[:, :width]))
    return jnp.concatenate(parts, axis=1)


def lower_mask():
    pick = lambda axis: lax.broadcasted_iota(jnp.int32, (SPAN, SPAN), axis)
    return pick(0) >= pick(1)


def states_kernel(first, head, x_ref, quarters_ref, dt_ref, rate_ref, cum_ref, enter_ref, message_ref, logs):
    rows, part = x_ref.shape[1:]
    segments, chunks = pl.num_programs(0), message_ref.shape[0]
    s = pl.program_id(0)
    lower = lower_mask().astype(F32)
    base = jnp.zeros_like(rate_ref[...])
    states = [None] * (part // head)
    for b in range(rows // SPAN):
        at = slice(b * SPAN, (b + 1) * SPAN)
        dt = dt_ref[0, at]
        cum = jnp.dot(
            lower, -dt * rate_ref[...], precision=lax.Precision.HIGHEST, preferred_element_type=F32
        )
        cum_ref[0, at] = cum
        b_cols = group_rows(quarters_ref, at, 0).T
        last = cum[SPAN - 1 : SPAN]
        base = base + last
        tail = jnp.exp(last - cum) * dt
        for h in range(part // head):
            lane = slice(first + h, first + h + 1)
            cols = slice(h * head, (h + 1) * head)
            wide = x_ref[0, at, cols].astype(F32)
            fresh = dot(b_cols, (wide * tail[:, lane]).astype(BF16))
            if b:
                enter_ref[0, b - 1, :, cols] = states[h]
                fresh = jnp.exp(last[:, lane]) * states[h] + fresh
            states[h] = fresh
    deep = states[0].shape[0] // chunks
    for h in range(part // head):
        cols = slice(h * head, (h + 1) * head)
        place = pl.ds(pl.multiple_of(s * deep, deep), deep)
        message_ref[:, place, cols] = states[h].reshape(chunks, deep, head).astype(BF16)
        log = jnp.broadcast_to(base[:, first + h : first + h + 1], (1, head))
        high = log.astype(BF16).astype(F32)
        row = lax.broadcasted_iota(jnp.int32, (logs.shape[0], head), 0)
        kept = jnp.where(row == 2 * s + 1, log - high, logs[:, cols])
        logs[:, cols] = jnp.where(row == 2 * s, high, kept)

    @pl.when(s == segments - 1)
    def _():
        tail_rows = logs[...].astype(BF16)
        for q in range(chunks):
            message_ref[q, message_ref.shape[1] - logs.shape[0] :, :] = tail_rows


def quarters_spec(quarters):
    return pl.BlockSpec((quarters.shape[0], 1, *quarters.shape[2:]), lambda s: (0, s // 2, 0, 0))


def block_states(x, quarters, dt, rate, first, head, chunks):
    segments, rows, part = x.shape
    n = quarters.shape[0] // 2 * quarters.shape[3] // 2
    message = (chunks, segments * n // chunks + 2 * segments, part)
    enter = jax.ShapeDtypeStruct((segments, rows // SPAN - 1, n, part), F32)
    return pl.pallas_call(
        functools.partial(states_kernel, first, head),
        grid=(segments,),
        in_specs=[each(x), quarters_spec(quarters), each(dt), whole(rate)],
        out_specs=[each(dt), each(enter), pl.BlockSpec(message, lambda s: (0, 0, 0))],
        out_shape=[
            jax.ShapeDtypeStruct(dt.shape, F32),
            enter,
            jax.ShapeDtypeStruct(message, BF16),
        ],
        scratch_shapes=[pltpu.VMEM((2 * segments, part), F32)],
        cost_estimate=cost(2 * x.size * n, x, dt, dt),
        name="block_states",
    )(x, quarters, dt, rate)


def intra_kernel(first, head, x_ref, quarters_ref, dt_ref, cum_ref, skip_ref, y_ref, c_ref):
    rows, part = x_ref.shape[1:]
    mask = lower_mask()
    for b in range(rows // SPAN):
        at = slice(b * SPAN, (b + 1) * SPAN)
        cum = cum_ref[0, at]
        cum_rows, dt_rows = cum.T, dt_ref[0, at].T
        c_block = group_rows(quarters_ref, at, 1)
        c_ref[0, at] = c_block
        scores = lax.dot_general(
            c_block,
            group_rows(quarters_ref, at, 0),
            (((1,), (1,)), ((), ())),
            preferred_element_type=F32,
        )
        for h in range(part // head):
            lane = slice(first + h, first + h + 1)
            cols = slice(h * head, (h + 1) * head)
            gap = cum[:, lane] - cum_rows[lane]
            decay = jnp.where(mask, jnp.exp(jnp.where(mask, gap, 0.0)), 0.0)
            mix = (scores * decay * dt_rows[lane]).astype(BF16)
            x = x_ref[0, at, cols]
            y_ref[0, at, cols] = dot(mix, x) + skip_ref[:, cols] * x.astype(F32)


def intra_blocks(x, quarters, dt, cum, skip, first, head):
    segments, rows, part = x.shape
    n = quarters.shape[0] // 2 * quarters.shape[3] // 2
    return pl.pallas_call(
        functools.partial(intra_kernel, first, head),
        grid=(segments,),
        in_specs=[each(x), quarters_spec(quarters), each(dt), each(cum), whole(skip)],
        out_specs=[each(x), pl.BlockSpec((1, rows, n), lambda s: (s, 0, 0))],
        out_shape=[
            jax.ShapeDtypeStruct(x.shape, F32),
            jax.ShapeDtypeStruct((segments, rows, n), BF16),
        ],
        cost_estimate=cost(64 * x.size * SPAN, x, x, x, dt, cum),
        name="intra_blocks",
    )(x, quarters, dt, cum, skip)


def combine_kernel(segments, r_ref, o_ref):
    places, part = r_ref.shape[0], r_ref.shape[2]
    deep = o_ref.shape[1] // segments
    logs = r_ref[:, segments * deep :, :].astype(F32)
    state = jnp.zeros((deep, part), F32)
    for s in range(segments):
        at = slice(s * deep, (s + 1) * deep)
        for z in range(places):
            o_ref[z, at] = state.astype(BF16)
            decay = jnp.exp(logs[z, 2 * s : 2 * s + 1] + logs[z, 2 * s + 1 : 2 * s + 2])
            state = decay * state + r_ref[z, at].astype(F32)


def combine_states(received, segments):
    places, deep, part = received.shape
    return pl.pallas_call(
        functools.partial(combine_kernel, segments),
        out_shape=jax.ShapeDtypeStruct((places, deep - 2 * segments, part), BF16),
        name="combine_states",
    )(received)


def gate_kernel(first, head, y_ref, cum_ref, c_ref, enter_ref, s_ref, z_ref, o_ref):
    rows, part = y_ref.shape[1:]
    incoming = s_ref[...].reshape(c_ref.shape[2], part).astype(F32)
    base = jnp.zeros_like(cum_ref[0, :1])
    for b in range(rows // SPAN):
        at = slice(b * SPAN, (b + 1) * SPAN)
        cum = cum_ref[0, at]
        for h in range(part // head):
            lane = slice(first + h, first + h + 1)
            cols = slice(h * head, (h + 1) * head)
            enter = incoming[:, cols]
            if b:
                enter = jnp.exp(base[:, lane]) * enter + enter_ref[0, b - 1, :, cols]
            inter = dot(c_ref[0, at], enter.astype(BF16))
            y = y_ref[0, at, cols] + jnp.exp(cum[:, lane]) * inter
            o_ref[0, at, cols] = (y * silu(z_ref[0, at, cols].astype(F32))).astype(BF16)
        base = base + cum[SPAN - 1 :]


def gate_blocks(y, cum, c, enter, entering, z, first, head):
    segments, rows, part = y.shape
    deep = entering.shape[1] // segments
    return pl.pallas_call(
        functools.partial(gate_kernel, first, head),
        grid=(segments,),
        in_specs=[
            each(y),
            each(cum),
            each(c),
            each(enter),
            pl.BlockSpec((entering.shape[0], deep, part), lambda s: (0, s, 0)),
            each(z),
        ],
        out_specs=each(z),
        out_shape=jax.ShapeDtypeStruct(z.shape, BF16),
        cost_estimate=cost(2 * z.size * c.shape[2], y, cum, c, enter, z, z),
        name="gate_blocks",
    )(y, cum, c, enter, entering, z)


def normed_kernel(side_ref, g_ref, gain_ref, w_ref, o_ref, normed_ref):
    quarters, rows, part = g_ref.shape

    @pl.when(pl.program_id(0) == 0)
    def _():
        squares = jnp.zeros((rows, part), F32)
        for q in range(quarters):
            g = g_ref[q].astype(F32)
            squares = squares + g * g
        squares = jnp.sum(squares, axis=1, keepdims=True)
        scale = lax.rsqrt(squares / (quarters * part) + EPS)
        for q in range(quarters):
            cols = slice(q * part, (q + 1) * part)
            normed_ref[:, cols] = (g_ref[q].astype(F32) * scale * gain_ref[:, cols]).astype(BF16)

    o_ref[0] = dot(normed_ref[...], w_ref[...]).astype(BF16)


def out_kernel(side_ref, normed_ref, w_ref, o_ref):
    o_ref[0] = dot(normed_ref[...], w_ref[...]).astype(BF16)


def out_partial(side, inputs, w, rows, places, sides):
    width = w.shape[1] // (places * sides)
    first = len(inputs) > 1
    keep = lambda a: pl.BlockSpec(a.shape, lambda i, s: (0,) * len(a.shape))
    normed = jax.ShapeDtypeStruct((rows, w.shape[0]), BF16)
    partial = jax.ShapeDtypeStruct((places, rows, width), BF16)
    partial_spec = pl.BlockSpec((1, rows, width), lambda i, s: (i, 0, 0))
    return pl.pallas_call(
        normed_kernel if first else out_kernel,
        grid_spec=pltpu.PrefetchScalarGridSpec(
            num_scalar_prefetch=1,
            grid=(places,),
            in_specs=[
                *(keep(a) for a in inputs),
                pl.BlockSpec((w.shape[0], width), lambda i, s: (0, i * sides + s[0])),
            ],
            out_specs=[partial_spec, keep(normed)] if first else partial_spec,
        ),
        out_shape=[partial, normed] if first else partial,
        cost_estimate=cost(w.size * rows, w, partial),
        name="out_normed" if first else "out_partial",
    )(jnp.full((1,), side, jnp.int32), *inputs, w)


def gathered_weights(packed, low, edge):
    nz, zi = lax.axis_size("z"), lax.axis_index("z")
    segments, depth, lanes = packed.shape
    blank = lambda width: jnp.zeros((segments, nz, depth, width), BF16)
    parts = [blank(low), blank(lanes - low)]

    def placed(which, block, distance):
        place = lax.rem(zi + distance + nz, nz)
        parts[which] = lax.dynamic_update_slice(parts[which], block[:, None], (0, place, 0, 0))

    def both(block, distance):
        placed(0, block[..., :low], distance)
        placed(1, block[..., low:], distance)

    left = right = packed
    both(packed, 0)
    for step in range(1, nz // 2):
        left, right = shifted(left, "z", 1), shifted(right, "z", -1)
        if step == 1:
            left, right, edge = lax.optimization_barrier((left, right, edge))
        both(left, -step)
        both(right, step)
    placed(0, shifted(left[..., :low], "z", 1), -(nz // 2))
    placed(1, shifted(right[..., low:], "z", -1), nz // 2)
    peers = lax.axis_size(("x", "y", "c"))
    edges = lax.all_to_all(
        jnp.broadcast_to(edge[None], (peers, *edge.shape)), ("x", "y", "c"), 0, 0, tiled=True
    )
    return *(p.reshape(segments * nz * depth, -1) for p in parts), edges


def local(
    hidden_in,
    norm_gain,
    w_x,
    w_z,
    w_bc,
    w_dt,
    dt_bias,
    decay_rate,
    conv_x,
    conv_bc,
    conv_bias_x,
    conv_bias_bc,
    skip_d,
    out_gain,
    w_out,
):
    nx, nz, ny, nc = (lax.axis_size(a) for a in ("x", "z", "y", "c"))
    xi, zi, ci = (lax.axis_index(a) for a in ("x", "z", "c"))
    rows, feats = hidden_in.shape
    depth, width = w_x.shape
    part = width // nx
    bc_width = w_bc.shape[2]
    bc_part = bc_width // nx
    heads = decay_rate.shape[0]
    own_heads = heads // nx
    taps = conv_x.shape[0]
    low = -(-(part + bc_part + own_heads) // 128) * 128
    spare = low - part - bc_part - own_heads

    gathered = lax.all_gather(hidden_in, ("x", "y", "c"), axis=0)
    gathered = gathered.reshape(nx, ny * nc, rows, feats)
    route = [(i, i + 1) for i in range(nx * nz - 1)]
    edge = lax.ppermute(hidden_in[rows - LEAD :], ("x", "z"), route)

    gain = lax.dynamic_slice(norm_gain, ((xi * nz + zi) * depth,), (depth,))
    pieces = [w.reshape(depth, nx, -1) for w in (w_x, w_bc, w_dt)]
    pieces.append(jnp.zeros((depth, nx, spare), BF16))
    pieces.append(w_z.reshape(depth, nx, part))
    packed = jnp.concatenate(pieces, axis=2).astype(F32) * gain[:, None, None]
    packed = jnp.transpose(packed.astype(BF16), (1, 0, 2))
    packed = lax.all_to_all(packed, "x", 0, 0, tiled=True)
    w_low, w_gate, edges = lax.optimization_barrier(gathered_weights(packed, low, edge))
    edges = edges.reshape(nx, ny * nc, LEAD, feats)

    def own(a):
        size = a.shape[-1] // nx
        return lax.dynamic_slice_in_dim(a, xi * size, size, axis=a.ndim - 1)

    row = lambda a: a.reshape(1, -1)
    tap_rows = jnp.concatenate([own(conv_x), own(conv_bc.reshape(taps, -1))], axis=1)
    tap_rows = jnp.pad(tap_rows, ((0, 0), (0, own_heads + spare)))
    bias_row = jnp.concatenate([own(conv_bias_x), own(conv_bias_bc.reshape(-1))])
    bias_row = row(jnp.pad(bias_row, (0, own_heads + spare)))
    in_lanes = lambda a: row(jnp.pad(own(a), (bc_part, spare)))
    x_conv, quarter, dt = project(
        edges, gathered, w_low, tap_rows, bias_row, in_lanes(dt_bias), part, bc_part
    )
    quarters, gate_z = lax.optimization_barrier(
        (lax.all_to_all(quarter, "x", 0, 0, tiled=True), project_gate(gathered, w_gate, dt))
    )

    head = width // heads
    skip_row = row(jnp.repeat(own(skip_d), head))
    cum, enter, message = block_states(
        x_conv, quarters, dt, in_lanes(decay_rate), bc_part, head, nz
    )
    received, (y, c_rows) = lax.optimization_barrier(
        (
            lax.all_to_all(message, "z", 0, 0, tiled=True),
            intra_blocks(x_conv, quarters, dt, cum, skip_row, bc_part, head),
        )
    )
    entering = lax.all_to_all(combine_states(received, nx), "z", 0, 0, tiled=True)
    gated = gate_blocks(y, cum, c_rows, enter, entering, gate_z, bc_part, head)
    gated = lax.all_to_all(gated, "x", 0, 0, tiled=True)

    theirs, normed = out_partial(1 - ci, (gated, row(out_gain)), w_out, rows, ny, nc)
    theirs = shifted(theirs, "c", 1)
    ours = out_partial(ci, (normed,), w_out, rows, ny, nc)
    ours = (ours.astype(F32) + theirs.astype(F32)).astype(BF16)
    shares = lax.all_to_all(ours, "y", 0, 0, tiled=True)
    summed = jnp.sum(shares.astype(F32), axis=0)
    return (hidden_in.astype(F32) + summed).astype(BF16)


def solution(mesh):
    sizes = mesh.shape
    devices = mesh.devices.reshape(4, sizes["seq"] // 4, sizes["tensor"] // 2, 2)
    split = Mesh(devices, ("x", "z", "y", "c"))
    seq, tensor = ("x", "z"), ("y", "c")
    in_specs = (
        P(seq, tensor),
        P(),
        P(seq, tensor),
        P(seq, tensor),
        P(seq, tensor, None),
        P(seq, tensor),
        P(tensor),
        P(tensor),
        P(None, tensor),
        P(None, tensor, None),
        P(tensor),
        P(tensor, None),
        P(tensor),
        P(tensor),
        P(tensor, None),
    )
    return jax.shard_map(
        local, mesh=split, in_specs=in_specs, out_specs=P(seq, tensor), check_vma=False
    )
```

```python
import functools

import jax
import jax.numpy as jnp
from jax import lax
from jax.experimental import pallas as pl
from jax.experimental.pallas import tpu as pltpu
from jax.sharding import Mesh
from jax.sharding import PartitionSpec as P

SPAN = 128
LEAD = 16
EPS = 1e-05
F32, BF16 = jnp.float32, jnp.bfloat16


def dot(a, b):
    return jnp.dot(a, b, preferred_element_type=F32)


def shifted(block, axis, distance):
    n = lax.axis_size(axis)
    return lax.ppermute(block, axis, [(i, (i + distance) % n) for i in range(n)])


def silu(v):
    return v * jax.nn.sigmoid(v)


def whole(a):
    return pl.BlockSpec(a.shape, lambda s: (0,) * a.ndim)


def each(a):
    return pl.BlockSpec((1, *a.shape[1:]), lambda s: (s,) + (0,) * (a.ndim - 1))


def cost(flops, *arrays):
    moved = sum(a.size * a.dtype.itemsize for a in arrays)
    return pl.CostEstimate(flops=flops, bytes_accessed=moved, transcendentals=0)


def block_copies(blocks, lanes, place_ref, w, sems):
    segments, depth = blocks[0].shape[:2]
    copies = []
    for b, block in enumerate(blocks):
        low = min(lanes, block.shape[2] - w.shape[1])
        for s in range(segments):
            row = pl.multiple_of((s * len(blocks) + place_ref[b]) * depth, depth)
            copies.append(
                pltpu.make_async_copy(
                    block.at[s, :, pl.ds(low, w.shape[1])],
                    w.at[pl.ds(row, depth), :],
                    sems.at[b, s],
                )
            )
    return copies


def proj_kernel(halves, count, place_ref, edge_ref, h_ref, *refs):
    blocks, refs = refs[:count], refs[count:]
    taps_ref, bias_ref, dt_bias_ref, x_ref, bc_ref, dt_ref, w_ref, acc, pre, sems = refs

    @pl.when(pl.program_id(0) == 0)
    def _():
        copies = block_copies(blocks, 0, place_ref, w_ref, sems)
        for copy in copies:
            copy.start()
        for copy in copies:
            copy.wait()

    pieces, feats = h_ref.shape[1], h_ref.shape[3]
    part, total = x_ref.shape[2], pieces * feats
    rows, bc_part = x_ref.shape[1], bc_ref.shape[3] // halves
    lanes = min(128, feats)
    step = pieces // 2
    squares = None
    for j in range(0, pieces, step):
        tall = []
        for i in range(j, j + step):
            h = jnp.concatenate([edge_ref[0, i], h_ref[0, i]], axis=0)
            tall.append(h)
            wide = h.astype(F32)
            for k in range(0, feats, lanes):
                square = wide[:, k : k + lanes] * wide[:, k : k + lanes]
                squares = square if squares is None else squares + square
        product = dot(jnp.concatenate(tall, axis=1), w_ref[j * feats : (j + step) * feats, :])
        if j == 0:
            acc[...] = product
        else:
            acc[...] += product
    scale = lax.rsqrt(jnp.sum(squares, axis=1, keepdims=True) / total + EPS)
    spare = dt_ref.shape[2]
    dt_raw = acc[LEAD:, part:] * scale[LEAD:] + dt_bias_ref[...]
    dt = jnp.maximum(dt_raw, 0.0) + jnp.log1p(jnp.exp(-jnp.abs(dt_raw)))
    lane = lax.broadcasted_iota(jnp.int32, dt.shape, 1)
    dt_ref[0] = jnp.where(lane == spare - 1, scale[LEAD:], dt)
    pre[...] = (acc[...] * scale).astype(BF16).astype(F32)
    taps = taps_ref.shape[0]
    running = bias_ref[...]
    for k in range(taps):
        start = LEAD - taps + 1 + k
        running = running + taps_ref[k : k + 1] * pre[start : start + rows]
    mixed = silu(running).astype(BF16)
    x_ref[0] = mixed[:, :part]
    quarter = mixed[:, part : part + bc_part]
    for side in range(halves):

        @pl.when(lax.rem(pl.program_id(0), halves) == side)
        def _():
            for q in range(bc_ref.shape[0]):
                bc_ref[q, 0, :, side * bc_part : (side + 1) * bc_part] = quarter


def project(place, edge, h, blocks, taps, bias, dt_bias, part, bc_part):
    segments, pieces, rows, feats = h.shape
    low, total = taps.shape[1], pieces * feats
    out = lambda width: pl.BlockSpec((1, rows, width), lambda s, p: (s, 0, 0))
    shape = lambda width, dtype: jax.ShapeDtypeStruct((segments, rows, width), dtype)
    keep = lambda a: pl.BlockSpec(a.shape, lambda s, p: (0,) * a.ndim)
    step = lambda a: pl.BlockSpec((1, *a.shape[1:]), lambda s, p: (s, 0, 0, 0))
    packed = (segments, segments // 2, rows, 2 * bc_part)
    return pl.pallas_call(
        functools.partial(proj_kernel, 2, len(blocks)),
        grid_spec=pltpu.PrefetchScalarGridSpec(
            num_scalar_prefetch=1,
            grid=(segments,),
            in_specs=[
                step(edge),
                step(h),
                *(pl.BlockSpec(memory_space=pl.ANY) for _ in blocks),
                keep(taps),
                keep(bias),
                keep(dt_bias),
            ],
            out_specs=[
                out(part),
                pl.BlockSpec((segments, 1, *packed[2:]), lambda s, p: (0, s // 2, 0, 0)),
                out(low - part),
            ],
            scratch_shapes=[
                pltpu.VMEM((total, low), BF16),
                pltpu.VMEM((rows + LEAD, low), F32),
                pltpu.VMEM((rows + LEAD, low), F32),
                pltpu.SemaphoreType.DMA((len(blocks), segments)),
            ],
        ),
        out_shape=[
            shape(part, BF16),
            jax.ShapeDtypeStruct(packed, BF16),
            shape(low - part, F32),
        ],
        cost_estimate=cost(2 * h.size * low, h),
        name="project",
    )(place, edge, h, *blocks, taps, bias, dt_bias)


def gate_proj_kernel(count, low, place_ref, h_ref, *refs):
    blocks, (dt_ref, z_ref, w_ref, sems) = refs[:count], refs[count:]

    @pl.when(pl.program_id(0) == 0)
    def _():
        copies = block_copies(blocks, low, place_ref, w_ref, sems)
        for copy in copies:
            copy.start()
        for copy in copies:
            copy.wait()

    pieces = h_ref.shape[1]
    tall = jnp.concatenate([h_ref[0, j] for j in range(pieces)], axis=1)
    scale = dt_ref[0, :, dt_ref.shape[2] - 1 :]
    z_ref[0] = (dot(tall, w_ref[...]) * scale).astype(BF16)


def project_gate(place, h, blocks, dt, low):
    segments, pieces, rows, feats = h.shape
    part = blocks[0].shape[2] - low
    return pl.pallas_call(
        functools.partial(gate_proj_kernel, len(blocks), low),
        grid_spec=pltpu.PrefetchScalarGridSpec(
            num_scalar_prefetch=1,
            grid=(segments,),
            in_specs=[
                pl.BlockSpec((1, pieces, rows, feats), lambda s, p: (s, 0, 0, 0)),
                *(pl.BlockSpec(memory_space=pl.ANY) for _ in blocks),
                pl.BlockSpec((1, *dt.shape[1:]), lambda s, p: (s, 0, 0)),
            ],
            out_specs=pl.BlockSpec((1, rows, part), lambda s, p: (s, 0, 0)),
            scratch_shapes=[
                pltpu.VMEM((pieces * feats, part), BF16),
                pltpu.SemaphoreType.DMA((len(blocks), segments)),
            ],
        ),
        out_shape=jax.ShapeDtypeStruct((segments, rows, part), BF16),
        cost_estimate=cost(2 * h.size * part, h),
        name="project_gate",
    )(place, h, *blocks, dt)


def group_rows(quarters_ref, at, first):
    count, width = quarters_ref.shape[0] // 2, quarters_ref.shape[3] // 2
    odd = lax.rem(pl.program_id(0), 2) == 1
    parts = []
    for q in range(count):
        pair = quarters_ref[first * count + q, 0, at]
        parts.append(jnp.where(odd, pair[:, width:], pair[:, :width]))
    return jnp.concatenate(parts, axis=1)


def lower_mask():
    pick = lambda axis: lax.broadcasted_iota(jnp.int32, (SPAN, SPAN), axis)
    return pick(0) >= pick(1)


def states_kernel(first, head, x_ref, quarters_ref, dt_ref, rate_ref, cum_ref, enter_ref, message_ref, logs):
    rows, part = x_ref.shape[1:]
    segments, chunks = pl.num_programs(0), message_ref.shape[0]
    s = pl.program_id(0)
    lower = lower_mask().astype(F32)
    base = jnp.zeros_like(rate_ref[...])
    states = [None] * (part // head)
    for b in range(rows // SPAN):
        at = slice(b * SPAN, (b + 1) * SPAN)
        dt = dt_ref[0, at]
        cum = jnp.dot(
            lower, -dt * rate_ref[...], precision=lax.Precision.HIGHEST, preferred_element_type=F32
        )
        cum_ref[0, at] = cum
        b_cols = group_rows(quarters_ref, at, 0).T
        last = cum[SPAN - 1 : SPAN]
        base = base + last
        tail = jnp.exp(last - cum) * dt
        for h in range(part // head):
            lane = slice(first + h, first + h + 1)
            cols = slice(h * head, (h + 1) * head)
            wide = x_ref[0, at, cols].astype(F32)
            fresh = dot(b_cols, (wide * tail[:, lane]).astype(BF16))
            if b:
                enter_ref[0, b - 1, :, cols] = states[h]
                fresh = jnp.exp(last[:, lane]) * states[h] + fresh
            states[h] = fresh
    deep = states[0].shape[0] // chunks
    for h in range(part // head):
        cols = slice(h * head, (h + 1) * head)
        place = pl.ds(pl.multiple_of(s * deep, deep), deep)
        message_ref[:, place, cols] = states[h].reshape(chunks, deep, head).astype(BF16)
        log = jnp.broadcast_to(base[:, first + h : first + h + 1], (1, head))
        high = log.astype(BF16).astype(F32)
        row = lax.broadcasted_iota(jnp.int32, (logs.shape[0], head), 0)
        kept = jnp.where(row == 2 * s + 1, log - high, logs[:, cols])
        logs[:, cols] = jnp.where(row == 2 * s, high, kept)

    @pl.when(s == segments - 1)
    def _():
        tail_rows = logs[...].astype(BF16)
        for q in range(chunks):
            message_ref[q, message_ref.shape[1] - logs.shape[0] :, :] = tail_rows


def quarters_spec(quarters):
    return pl.BlockSpec((quarters.shape[0], 1, *quarters.shape[2:]), lambda s: (0, s // 2, 0, 0))


def block_states(x, quarters, dt, rate, first, head, chunks):
    segments, rows, part = x.shape
    n = quarters.shape[0] // 2 * quarters.shape[3] // 2
    message = (chunks, segments * n // chunks + 2 * segments, part)
    enter = jax.ShapeDtypeStruct((segments, rows // SPAN - 1, n, part), F32)
    return pl.pallas_call(
        functools.partial(states_kernel, first, head),
        grid=(segments,),
        in_specs=[each(x), quarters_spec(quarters), each(dt), whole(rate)],
        out_specs=[each(dt), each(enter), pl.BlockSpec(message, lambda s: (0, 0, 0))],
        out_shape=[
            jax.ShapeDtypeStruct(dt.shape, F32),
            enter,
            jax.ShapeDtypeStruct(message, BF16),
        ],
        scratch_shapes=[pltpu.VMEM((2 * segments, part), F32)],
        cost_estimate=cost(2 * x.size * n, x, dt, dt),
        name="block_states",
    )(x, quarters, dt, rate)


def intra_kernel(first, head, x_ref, quarters_ref, dt_ref, cum_ref, skip_ref, y_ref, c_ref):
    rows, part = x_ref.shape[1:]
    mask = lower_mask()
    for b in range(rows // SPAN):
        at = slice(b * SPAN, (b + 1) * SPAN)
        cum = cum_ref[0, at]
        cum_rows, dt_rows = cum.T, dt_ref[0, at].T
        c_block = group_rows(quarters_ref, at, 1)
        c_ref[0, at] = c_block
        scores = lax.dot_general(
            c_block,
            group_rows(quarters_ref, at, 0),
            (((1,), (1,)), ((), ())),
            preferred_element_type=F32,
        )
        for h in range(part // head):
            lane = slice(first + h, first + h + 1)
            cols = slice(h * head, (h + 1) * head)
            gap = cum[:, lane] - cum_rows[lane]
            decay = jnp.where(mask, jnp.exp(jnp.where(mask, gap, 0.0)), 0.0)
            mix = (scores * decay * dt_rows[lane]).astype(BF16)
            x = x_ref[0, at, cols]
            y_ref[0, at, cols] = dot(mix, x) + skip_ref[:, cols] * x.astype(F32)


def intra_blocks(x, quarters, dt, cum, skip, first, head):
    segments, rows, part = x.shape
    n = quarters.shape[0] // 2 * quarters.shape[3] // 2
    return pl.pallas_call(
        functools.partial(intra_kernel, first, head),
        grid=(segments,),
        in_specs=[each(x), quarters_spec(quarters), each(dt), each(cum), whole(skip)],
        out_specs=[each(x), pl.BlockSpec((1, rows, n), lambda s: (s, 0, 0))],
        out_shape=[
            jax.ShapeDtypeStruct(x.shape, F32),
            jax.ShapeDtypeStruct((segments, rows, n), BF16),
        ],
        cost_estimate=cost(64 * x.size * SPAN, x, x, x, dt, cum),
        name="intra_blocks",
    )(x, quarters, dt, cum, skip)


def combine_kernel(segments, r_ref, o_ref):
    places, part = r_ref.shape[0], r_ref.shape[2]
    deep = o_ref.shape[1] // segments
    logs = r_ref[:, segments * deep :, :].astype(F32)
    state = jnp.zeros((deep, part), F32)
    for s in range(segments):
        at = slice(s * deep, (s + 1) * deep)
        for z in range(places):
            o_ref[z, at] = state.astype(BF16)
            decay = jnp.exp(logs[z, 2 * s : 2 * s + 1] + logs[z, 2 * s + 1 : 2 * s + 2])
            state = decay * state + r_ref[z, at].astype(F32)


def combine_states(received, segments):
    places, deep, part = received.shape
    return pl.pallas_call(
        functools.partial(combine_kernel, segments),
        out_shape=jax.ShapeDtypeStruct((places, deep - 2 * segments, part), BF16),
        name="combine_states",
    )(received)


def gate_kernel(first, head, y_ref, cum_ref, c_ref, enter_ref, s_ref, z_ref, o_ref):
    rows, part = y_ref.shape[1:]
    incoming = s_ref[...].reshape(c_ref.shape[2], part).astype(F32)
    base = jnp.zeros_like(cum_ref[0, :1])
    for b in range(rows // SPAN):
        at = slice(b * SPAN, (b + 1) * SPAN)
        cum = cum_ref[0, at]
        for h in range(part // head):
            lane = slice(first + h, first + h + 1)
            cols = slice(h * head, (h + 1) * head)
            enter = incoming[:, cols]
            if b:
                enter = jnp.exp(base[:, lane]) * enter + enter_ref[0, b - 1, :, cols]
            inter = dot(c_ref[0, at], enter.astype(BF16))
            y = y_ref[0, at, cols] + jnp.exp(cum[:, lane]) * inter
            o_ref[0, at, cols] = (y * silu(z_ref[0, at, cols].astype(F32))).astype(BF16)
        base = base + cum[SPAN - 1 :]


def gate_blocks(y, cum, c, enter, entering, z, first, head):
    segments, rows, part = y.shape
    deep = entering.shape[1] // segments
    return pl.pallas_call(
        functools.partial(gate_kernel, first, head),
        grid=(segments,),
        in_specs=[
            each(y),
            each(cum),
            each(c),
            each(enter),
            pl.BlockSpec((entering.shape[0], deep, part), lambda s: (0, s, 0)),
            each(z),
        ],
        out_specs=each(z),
        out_shape=jax.ShapeDtypeStruct(z.shape, BF16),
        cost_estimate=cost(2 * z.size * c.shape[2], y, cum, c, enter, z, z),
        name="gate_blocks",
    )(y, cum, c, enter, entering, z)


def normed_kernel(tile_ref, g_ref, gain_ref, w_ref, first_ref, second_ref, normed_ref):
    quarters, rows, part = g_ref.shape

    @pl.when(pl.program_id(0) == 0)
    def _():
        squares = jnp.zeros((rows, part), F32)
        for q in range(quarters):
            g = g_ref[q].astype(F32)
            squares = squares + g * g
        squares = jnp.sum(squares, axis=1, keepdims=True)
        scale = lax.rsqrt(squares / (quarters * part) + EPS)
        for q in range(quarters):
            cols = slice(q * part, (q + 1) * part)
            normed_ref[:, cols] = (g_ref[q].astype(F32) * scale * gain_ref[:, cols]).astype(BF16)

    for side, o_ref in enumerate((first_ref, second_ref)):

        @pl.when(pl.program_id(0) == side)
        def _():
            o_ref[...] = dot(normed_ref[...], w_ref[...]).astype(BF16)


def out_kernel(tile_ref, normed_ref, w_ref, o_ref):
    o_ref[0] = dot(normed_ref[...], w_ref[...]).astype(BF16)


def out_partial(tiles, inputs, w, rows, width):
    count = tiles.shape[0]
    first = len(inputs) > 1
    keep = lambda a: pl.BlockSpec(a.shape, lambda i, t: (0,) * len(a.shape))
    normed = jax.ShapeDtypeStruct((rows, w.shape[0]), BF16)
    one = jax.ShapeDtypeStruct((rows, width), BF16)
    partial = jax.ShapeDtypeStruct((count, rows, width), BF16)
    partial_spec = pl.BlockSpec((1, rows, width), lambda i, t: (i, 0, 0))
    return pl.pallas_call(
        normed_kernel if first else out_kernel,
        grid_spec=pltpu.PrefetchScalarGridSpec(
            num_scalar_prefetch=1,
            grid=(count,),
            in_specs=[
                *(keep(a) for a in inputs),
                pl.BlockSpec((w.shape[0], width), lambda i, t: (0, t[i])),
            ],
            out_specs=[keep(one), keep(one), keep(normed)] if first else partial_spec,
        ),
        out_shape=[one, one, normed] if first else partial,
        cost_estimate=cost(2 * w.shape[0] * rows * width * count, partial, normed),
        name="out_normed" if first else "out_partial",
    )(tiles, *inputs, w)


def out_shares(gated, gain, w, feats):
    rows = gated.shape[1]
    nc, ny = lax.axis_size("c"), lax.axis_size("y")
    ci, yi = lax.axis_index("c"), lax.axis_index("y")

    def tile(distance, side):
        return lax.rem(yi + distance, ny) * nc + side

    mine, other = ci, 1 - ci
    tiles = lambda *pairs: jnp.stack([tile(d, side) for d, side in pairs])
    far_other, far, normed = out_partial(
        tiles((2, other), (2, mine)), (gated, gain), w, rows, feats
    )
    far_other = shifted(far_other, "c", 1)
    near_other = out_partial(
        tiles((1, other), (3, other), (0, other)), (normed,), w, rows, feats
    )
    near_other = shifted(near_other, "c", 1)
    far = (far.astype(F32) + far_other.astype(F32)).astype(BF16)
    upper = shifted(far[: rows // 2], "y", 1)
    lower = shifted(far[rows // 2 :], "y", -1)
    near = out_partial(tiles((1, mine), (3, mine), (0, mine)), (normed,), w, rows, feats)
    blank = jnp.zeros((rows // 2, feats), F32)
    near = [n.astype(F32) + o.astype(F32) for n, o in zip(near, near_other)]
    up = near[0] + jnp.concatenate([upper.astype(F32), blank], axis=0)
    down = near[1] + jnp.concatenate([blank, lower.astype(F32)], axis=0)
    up, down = shifted(up.astype(BF16), "y", 1), shifted(down.astype(BF16), "y", -1)
    return near[2] + up.astype(F32) + down.astype(F32)


def gathered_weights(packed, low, edge):
    nz, zi = lax.axis_size("z"), lax.axis_index("z")
    half = nz // 2
    left = right = packed
    blocks, distances = [packed], [0]
    for step in range(1, half):
        left, right = shifted(left, "z", 1), shifted(right, "z", -1)
        if step == 1:
            left, right, edge = lax.optimization_barrier((left, right, edge))
        blocks += [left, right]
        distances += [-step, step]
    far_low = shifted(left[..., :low], "z", 1)
    far_gate = shifted(right[..., low:], "z", -1)
    place = lax.rem(zi + jnp.array([*distances, half], jnp.int32) + nz, nz)
    peers = lax.axis_size(("x", "y", "c"))
    edges = lax.all_to_all(
        jnp.broadcast_to(edge[None], (peers, *edge.shape)), ("x", "y", "c"), 0, 0, tiled=True
    )
    return place, (*blocks, far_low), (*blocks, far_gate), edges


def local(
    hidden_in,
    norm_gain,
    w_x,
    w_z,
    w_bc,
    w_dt,
    dt_bias,
    decay_rate,
    conv_x,
    conv_bc,
    conv_bias_x,
    conv_bias_bc,
    skip_d,
    out_gain,
    w_out,
):
    nx, nz, ny, nc = (lax.axis_size(a) for a in ("x", "z", "y", "c"))
    xi, zi = (lax.axis_index(a) for a in ("x", "z"))
    rows, feats = hidden_in.shape
    depth, width = w_x.shape
    part = width // nx
    bc_width = w_bc.shape[2]
    bc_part = bc_width // nx
    heads = decay_rate.shape[0]
    own_heads = heads // nx
    taps = conv_x.shape[0]
    low = -(-(part + bc_part + own_heads) // 128) * 128
    spare = low - part - bc_part - own_heads

    gathered = lax.all_gather(hidden_in, ("x", "y", "c"), axis=0)
    gathered = gathered.reshape(nx, ny * nc, rows, feats)
    route = [(i, i + 1) for i in range(nx * nz - 1)]
    edge = lax.ppermute(hidden_in[rows - LEAD :], ("x", "z"), route)

    gain = lax.dynamic_slice(norm_gain, ((xi * nz + zi) * depth,), (depth,))
    pieces = [w.reshape(depth, nx, -1) for w in (w_x, w_bc, w_dt)]
    pieces.append(jnp.zeros((depth, nx, spare), BF16))
    pieces.append(w_z.reshape(depth, nx, part))
    packed = jnp.concatenate(pieces, axis=2).astype(F32) * gain[:, None, None]
    packed = jnp.transpose(packed.astype(BF16), (1, 0, 2))
    packed = lax.all_to_all(packed, "x", 0, 0, tiled=True)
    place, w_low, w_gate, edges = lax.optimization_barrier(gathered_weights(packed, low, edge))
    edges = edges.reshape(nx, ny * nc, LEAD, feats)

    def own(a):
        size = a.shape[-1] // nx
        return lax.dynamic_slice_in_dim(a, xi * size, size, axis=a.ndim - 1)

    row = lambda a: a.reshape(1, -1)
    tap_rows = jnp.concatenate([own(conv_x), own(conv_bc.reshape(taps, -1))], axis=1)
    tap_rows = jnp.pad(tap_rows, ((0, 0), (0, own_heads + spare)))
    bias_row = jnp.concatenate([own(conv_bias_x), own(conv_bias_bc.reshape(-1))])
    bias_row = row(jnp.pad(bias_row, (0, own_heads + spare)))
    in_lanes = lambda a: row(jnp.pad(own(a), (bc_part, spare)))
    x_conv, quarter, dt = project(
        place, edges, gathered, w_low, tap_rows, bias_row, in_lanes(dt_bias), part, bc_part
    )
    quarters = lax.all_to_all(quarter, "x", 0, 0, tiled=True)

    head = width // heads
    skip_row = row(jnp.repeat(own(skip_d), head))
    cum, enter, message = block_states(
        x_conv, quarters, dt, in_lanes(decay_rate), bc_part, head, nz
    )
    received, (y, c_rows) = lax.optimization_barrier(
        (
            lax.all_to_all(message, "z", 0, 0, tiled=True),
            intra_blocks(x_conv, quarters, dt, cum, skip_row, bc_part, head),
        )
    )
    states = combine_states(received, nx)
    states, gate_inputs = lax.optimization_barrier((states, gathered))
    entering, gate_z = lax.optimization_barrier(
        (
            lax.all_to_all(states, "z", 0, 0, tiled=True),
            project_gate(place, gate_inputs, w_gate, dt, low),
        )
    )
    gated = gate_blocks(y, cum, c_rows, enter, entering, gate_z, bc_part, head)
    gated = lax.all_to_all(gated, "x", 0, 0, tiled=True)

    summed = out_shares(gated, row(out_gain), w_out, feats)
    return (hidden_in.astype(F32) + summed).astype(BF16)


def solution(mesh):
    sizes = mesh.shape
    devices = mesh.devices.reshape(4, sizes["seq"] // 4, sizes["tensor"] // 2, 2)
    split = Mesh(devices, ("x", "z", "y", "c"))
    seq, tensor = ("x", "z"), ("y", "c")
    in_specs = (
        P(seq, tensor),
        P(),
        P(seq, tensor),
        P(seq, tensor),
        P(seq, tensor, None),
        P(seq, tensor),
        P(tensor),
        P(tensor),
        P(None, tensor),
        P(None, tensor, None),
        P(tensor),
        P(tensor, None),
        P(tensor),
        P(tensor),
        P(tensor, None),
    )
    return jax.shard_map(
        local, mesh=split, in_specs=in_specs, out_specs=P(seq, tensor), check_vma=False
    )
```

```python
import functools

import jax
import jax.numpy as jnp
from jax import lax
from jax.experimental import pallas as pl
from jax.experimental.pallas import tpu as pltpu
from jax.sharding import Mesh
from jax.sharding import PartitionSpec as P

SPAN = 128
LEAD = 16
EPS = 1e-05
F32, BF16 = jnp.float32, jnp.bfloat16


def dot(a, b):
    return jnp.dot(a, b, preferred_element_type=F32)


def shifted(block, axis, distance):
    n = lax.axis_size(axis)
    return lax.ppermute(block, axis, [(i, (i + distance) % n) for i in range(n)])


def silu(v):
    return v * jax.nn.sigmoid(v)


def whole(a):
    return pl.BlockSpec(a.shape, lambda s: (0,) * a.ndim)


def each(a):
    return pl.BlockSpec((1, *a.shape[1:]), lambda s: (s,) + (0,) * (a.ndim - 1))


def cost(flops, *arrays):
    moved = sum(a.size * a.dtype.itemsize for a in arrays)
    return pl.CostEstimate(flops=flops, bytes_accessed=moved, transcendentals=0)


def block_copies(blocks, lanes, place_ref, w, sems):
    segments, depth = blocks[0].shape[:2]
    copies = []
    for b, block in enumerate(blocks):
        low = min(lanes, block.shape[2] - w.shape[1])
        for s in range(segments):
            row = pl.multiple_of((s * len(blocks) + place_ref[b]) * depth, depth)
            copies.append(
                pltpu.make_async_copy(
                    block.at[s, :, pl.ds(low, w.shape[1])],
                    w.at[pl.ds(row, depth), :],
                    sems.at[b, s],
                )
            )
    return copies


def proj_kernel(halves, count, place_ref, edge_ref, h_ref, *refs):
    blocks, refs = refs[:count], refs[count:]
    taps_ref, bias_ref, dt_bias_ref, x_ref, bc_ref, dt_ref, w_ref, acc, pre, sems = refs

    @pl.when(pl.program_id(0) == 0)
    def _():
        copies = block_copies(blocks, 0, place_ref, w_ref, sems)
        for copy in copies:
            copy.start()
        for copy in copies:
            copy.wait()

    pieces, feats = h_ref.shape[1], h_ref.shape[3]
    part, total = x_ref.shape[2], pieces * feats
    rows, bc_part = x_ref.shape[1], bc_ref.shape[3] // halves
    lanes = min(128, feats)
    step = pieces // 2
    squares = None
    for j in range(0, pieces, step):
        tall = []
        for i in range(j, j + step):
            h = jnp.concatenate([edge_ref[0, i], h_ref[0, i]], axis=0)
            tall.append(h)
            wide = h.astype(F32)
            for k in range(0, feats, lanes):
                square = wide[:, k : k + lanes] * wide[:, k : k + lanes]
                squares = square if squares is None else squares + square
        product = dot(jnp.concatenate(tall, axis=1), w_ref[j * feats : (j + step) * feats, :])
        if j == 0:
            acc[...] = product
        else:
            acc[...] += product
    scale = lax.rsqrt(jnp.sum(squares, axis=1, keepdims=True) / total + EPS)
    spare = dt_ref.shape[2]
    dt_raw = acc[LEAD:, part:] * scale[LEAD:] + dt_bias_ref[...]
    dt = jnp.maximum(dt_raw, 0.0) + jnp.log1p(jnp.exp(-jnp.abs(dt_raw)))
    lane = lax.broadcasted_iota(jnp.int32, dt.shape, 1)
    dt_ref[0] = jnp.where(lane == spare - 1, scale[LEAD:], dt)
    pre[...] = (acc[...] * scale).astype(BF16).astype(F32)
    taps = taps_ref.shape[0]
    running = bias_ref[...]
    for k in range(taps):
        start = LEAD - taps + 1 + k
        running = running + taps_ref[k : k + 1] * pre[start : start + rows]
    mixed = silu(running).astype(BF16)
    x_ref[0] = mixed[:, :part]
    quarter = mixed[:, part : part + bc_part]
    for side in range(halves):

        @pl.when(lax.rem(pl.program_id(0), halves) == side)
        def _():
            for q in range(bc_ref.shape[0]):
                bc_ref[q, 0, :, side * bc_part : (side + 1) * bc_part] = quarter


def project(place, edge, h, blocks, taps, bias, dt_bias, part, bc_part):
    segments, pieces, rows, feats = h.shape
    low, total = taps.shape[1], pieces * feats
    out = lambda width: pl.BlockSpec((1, rows, width), lambda s, p: (s, 0, 0))
    shape = lambda width, dtype: jax.ShapeDtypeStruct((segments, rows, width), dtype)
    keep = lambda a: pl.BlockSpec(a.shape, lambda s, p: (0,) * a.ndim)
    step = lambda a: pl.BlockSpec((1, *a.shape[1:]), lambda s, p: (s, 0, 0, 0))
    packed = (segments, segments // 2, rows, 2 * bc_part)
    return pl.pallas_call(
        functools.partial(proj_kernel, 2, len(blocks)),
        grid_spec=pltpu.PrefetchScalarGridSpec(
            num_scalar_prefetch=1,
            grid=(segments,),
            in_specs=[
                step(edge),
                step(h),
                *(pl.BlockSpec(memory_space=pl.ANY) for _ in blocks),
                keep(taps),
                keep(bias),
                keep(dt_bias),
            ],
            out_specs=[
                out(part),
                pl.BlockSpec((segments, 1, *packed[2:]), lambda s, p: (0, s // 2, 0, 0)),
                out(low - part),
            ],
            scratch_shapes=[
                pltpu.VMEM((total, low), BF16),
                pltpu.VMEM((rows + LEAD, low), F32),
                pltpu.VMEM((rows + LEAD, low), F32),
                pltpu.SemaphoreType.DMA((len(blocks), segments)),
            ],
        ),
        out_shape=[
            shape(part, BF16),
            jax.ShapeDtypeStruct(packed, BF16),
            shape(low - part, F32),
        ],
        cost_estimate=cost(2 * h.size * low, h),
        name="project",
    )(place, edge, h, *blocks, taps, bias, dt_bias)


def gate_proj_kernel(count, low, place_ref, h_ref, *refs):
    blocks, (dt_ref, z_ref, w_ref, sems) = refs[:count], refs[count:]

    @pl.when(pl.program_id(0) == 0)
    def _():
        copies = block_copies(blocks, low, place_ref, w_ref, sems)
        for copy in copies:
            copy.start()
        for copy in copies:
            copy.wait()

    pieces = h_ref.shape[1]
    tall = jnp.concatenate([h_ref[0, j] for j in range(pieces)], axis=1)
    scale = dt_ref[0, :, dt_ref.shape[2] - 1 :]
    z_ref[0] = (dot(tall, w_ref[...]) * scale).astype(BF16)


def project_gate(place, h, blocks, dt, low, start, count):
    pieces, rows, feats = h.shape[1:]
    part = blocks[0].shape[2] - low
    return pl.pallas_call(
        functools.partial(gate_proj_kernel, len(blocks), low),
        grid_spec=pltpu.PrefetchScalarGridSpec(
            num_scalar_prefetch=1,
            grid=(count,),
            in_specs=[
                pl.BlockSpec((1, pieces, rows, feats), lambda s, p: (s + start, 0, 0, 0)),
                *(pl.BlockSpec(memory_space=pl.ANY) for _ in blocks),
                pl.BlockSpec((1, *dt.shape[1:]), lambda s, p: (s + start, 0, 0)),
            ],
            out_specs=pl.BlockSpec((1, rows, part), lambda s, p: (s, 0, 0)),
            scratch_shapes=[
                pltpu.VMEM((pieces * feats, part), BF16),
                pltpu.SemaphoreType.DMA((len(blocks), blocks[0].shape[0])),
            ],
        ),
        out_shape=jax.ShapeDtypeStruct((count, rows, part), BF16),
        cost_estimate=cost(2 * h.size * part * count // h.shape[0], h),
        name="project_gate",
    )(place, h, *blocks, dt)


def group_rows(quarters_ref, at, first):
    count, width = quarters_ref.shape[0] // 2, quarters_ref.shape[3] // 2
    odd = lax.rem(pl.program_id(0), 2) == 1
    parts = []
    for q in range(count):
        pair = quarters_ref[first * count + q, 0, at]
        parts.append(jnp.where(odd, pair[:, width:], pair[:, :width]))
    return jnp.concatenate(parts, axis=1)


def lower_mask():
    pick = lambda axis: lax.broadcasted_iota(jnp.int32, (SPAN, SPAN), axis)
    return pick(0) >= pick(1)


def decay_kernel(first, head, x_ref, dt_ref, rate_ref, cum_ref, scaled_ref):
    rows, part = x_ref.shape[1:]
    lower = lower_mask().astype(F32)
    for b in range(rows // SPAN):
        at = slice(b * SPAN, (b + 1) * SPAN)
        dt = dt_ref[0, at]
        cum = jnp.dot(
            lower, -dt * rate_ref[...], precision=lax.Precision.HIGHEST, preferred_element_type=F32
        )
        cum_ref[0, at] = cum
        tail = jnp.exp(cum[SPAN - 1 : SPAN] - cum) * dt
        for h in range(part // head):
            cols = slice(h * head, (h + 1) * head)
            wide = x_ref[0, at, cols].astype(F32)
            scaled_ref[0, at, cols] = (wide * tail[:, first + h : first + h + 1]).astype(BF16)


def block_decays(x, dt, rate, first, head):
    return pl.pallas_call(
        functools.partial(decay_kernel, first, head),
        grid=(x.shape[0],),
        in_specs=[each(x), each(dt), whole(rate)],
        out_specs=[each(dt), each(x)],
        out_shape=[
            jax.ShapeDtypeStruct(dt.shape, F32),
            jax.ShapeDtypeStruct(x.shape, BF16),
        ],
        cost_estimate=cost(16 * dt.size * SPAN, x, x, dt, dt),
        name="block_decays",
    )(x, dt, rate)


def states_kernel(first, head, scaled_ref, quarters_ref, cum_ref, enter_ref, message_ref, logs):
    rows, part = scaled_ref.shape[1:]
    segments, chunks = pl.num_programs(0), message_ref.shape[0]
    s = pl.program_id(0)
    base = jnp.zeros_like(cum_ref[0, :1])
    state = None
    for b in range(rows // SPAN):
        at = slice(b * SPAN, (b + 1) * SPAN)
        last = cum_ref[0, (b + 1) * SPAN - 1 : (b + 1) * SPAN]
        base = base + last
        fresh = dot(group_rows(quarters_ref, at, 0).T, scaled_ref[0, at])
        if b:
            enter_ref[0, b - 1] = state
            decay = [
                jnp.broadcast_to(jnp.exp(last[:, first + h : first + h + 1]), (1, head))
                for h in range(part // head)
            ]
            fresh = jnp.concatenate(decay, axis=1) * state + fresh
        state = fresh
    deep = state.shape[0] // chunks
    place = pl.ds(pl.multiple_of(s * deep, deep), deep)
    message_ref[:, place, :] = state.reshape(chunks, deep, part).astype(BF16)
    for h in range(part // head):
        cols = slice(h * head, (h + 1) * head)
        log = jnp.broadcast_to(base[:, first + h : first + h + 1], (1, head))
        high = log.astype(BF16).astype(F32)
        row = lax.broadcasted_iota(jnp.int32, (logs.shape[0], head), 0)
        kept = jnp.where(row == 2 * s + 1, log - high, logs[:, cols])
        logs[:, cols] = jnp.where(row == 2 * s, high, kept)

    @pl.when(s == segments - 1)
    def _():
        tail_rows = logs[...].astype(BF16)
        for q in range(chunks):
            message_ref[q, message_ref.shape[1] - logs.shape[0] :, :] = tail_rows


def quarters_spec(quarters):
    return pl.BlockSpec((quarters.shape[0], 1, *quarters.shape[2:]), lambda s: (0, s // 2, 0, 0))


def block_states(scaled, quarters, cum, first, head, chunks):
    segments, rows, part = scaled.shape
    n = quarters.shape[0] // 2 * quarters.shape[3] // 2
    message = (chunks, segments * n // chunks + 2 * segments, part)
    enter = jax.ShapeDtypeStruct((segments, rows // SPAN - 1, n, part), F32)
    return pl.pallas_call(
        functools.partial(states_kernel, first, head),
        grid=(segments,),
        in_specs=[each(scaled), quarters_spec(quarters), each(cum)],
        out_specs=[each(enter), pl.BlockSpec(message, lambda s: (0, 0, 0))],
        out_shape=[enter, jax.ShapeDtypeStruct(message, BF16)],
        scratch_shapes=[pltpu.VMEM((2 * segments, part), F32)],
        cost_estimate=cost(2 * scaled.size * n, scaled, cum, enter),
        name="block_states",
    )(scaled, quarters, cum)


def intra_kernel(first, head, x_ref, quarters_ref, dt_ref, cum_ref, skip_ref, y_ref, c_ref):
    rows, part = x_ref.shape[1:]
    mask = lower_mask()
    for b in range(rows // SPAN):
        at = slice(b * SPAN, (b + 1) * SPAN)
        cum = cum_ref[0, at]
        cum_rows, dt_rows = cum.T, dt_ref[0, at].T
        c_block = group_rows(quarters_ref, at, 1)
        c_ref[0, at] = c_block
        scores = lax.dot_general(
            c_block,
            group_rows(quarters_ref, at, 0),
            (((1,), (1,)), ((), ())),
            preferred_element_type=F32,
        )
        for h in range(part // head):
            lane = slice(first + h, first + h + 1)
            cols = slice(h * head, (h + 1) * head)
            gap = cum[:, lane] - cum_rows[lane]
            decay = jnp.where(mask, jnp.exp(jnp.where(mask, gap, 0.0)), 0.0)
            mix = (scores * decay * dt_rows[lane]).astype(BF16)
            x = x_ref[0, at, cols]
            y_ref[0, at, cols] = dot(mix, x) + skip_ref[:, cols] * x.astype(F32)


def intra_blocks(x, quarters, dt, cum, skip, first, head):
    segments, rows, _ = x.shape
    n = quarters.shape[0] // 2 * quarters.shape[3] // 2
    return pl.pallas_call(
        functools.partial(intra_kernel, first, head),
        grid=(segments,),
        in_specs=[each(x), quarters_spec(quarters), each(dt), each(cum), whole(skip)],
        out_specs=[each(x), pl.BlockSpec((1, rows, n), lambda s: (s, 0, 0))],
        out_shape=[
            jax.ShapeDtypeStruct(x.shape, F32),
            jax.ShapeDtypeStruct((segments, rows, n), BF16),
        ],
        cost_estimate=cost(64 * x.size * SPAN, x, x, x, dt, cum),
        name="intra_blocks",
    )(x, quarters, dt, cum, skip)


def combine_kernel(segments, r_ref, o_ref):
    places, part = r_ref.shape[0], r_ref.shape[2]
    deep = o_ref.shape[1] // segments
    logs = r_ref[:, segments * deep :, :].astype(F32)
    state = jnp.zeros((deep, part), F32)
    for s in range(segments):
        at = slice(s * deep, (s + 1) * deep)
        for z in range(places):
            o_ref[z, at] = state.astype(BF16)
            decay = jnp.exp(logs[z, 2 * s : 2 * s + 1] + logs[z, 2 * s + 1 : 2 * s + 2])
            state = decay * state + r_ref[z, at].astype(F32)


def combine_states(received, segments):
    places, deep, part = received.shape
    return pl.pallas_call(
        functools.partial(combine_kernel, segments),
        out_shape=jax.ShapeDtypeStruct((places, deep - 2 * segments, part), BF16),
        name="combine_states",
    )(received)


def gate_kernel(first, head, half, y_ref, cum_ref, c_ref, enter_ref, s_ref, z0_ref, z1_ref, o_ref):
    rows, part = y_ref.shape[1:]
    incoming = s_ref[...].reshape(c_ref.shape[2], part).astype(F32)
    base = jnp.zeros_like(cum_ref[0, :1])
    for b in range(rows // SPAN):
        at = slice(b * SPAN, (b + 1) * SPAN)
        cum = cum_ref[0, at]
        for h in range(part // head):
            lane = slice(first + h, first + h + 1)
            cols = slice(h * head, (h + 1) * head)
            enter = incoming[:, cols]
            if b:
                enter = jnp.exp(base[:, lane]) * enter + enter_ref[0, b - 1, :, cols]
            inter = dot(c_ref[0, at], enter.astype(BF16))
            y = y_ref[0, at, cols] + jnp.exp(cum[:, lane]) * inter
            early = pl.program_id(0) < half
            z = jnp.where(early, z0_ref[0, at, cols], z1_ref[0, at, cols]).astype(F32)
            o_ref[0, at, cols] = (y * silu(z)).astype(BF16)
        base = base + cum[SPAN - 1 :]


def gate_blocks(y, cum, c, enter, entering, gates, first, head):
    segments, rows, part = y.shape
    deep = entering.shape[1] // segments
    half = gates[0].shape[0]
    out = jax.ShapeDtypeStruct(y.shape, BF16)
    return pl.pallas_call(
        functools.partial(gate_kernel, first, head, half),
        grid=(segments,),
        in_specs=[
            each(y),
            each(cum),
            each(c),
            each(enter),
            pl.BlockSpec((entering.shape[0], deep, part), lambda s: (0, s, 0)),
            pl.BlockSpec((1, rows, part), lambda s: (jnp.minimum(s, half - 1), 0, 0)),
            pl.BlockSpec((1, rows, part), lambda s: (jnp.maximum(s - half, 0), 0, 0)),
        ],
        out_specs=each(out),
        out_shape=out,
        cost_estimate=cost(2 * y.size * c.shape[2], y, cum, c, enter, out, out),
        name="gate_blocks",
    )(y, cum, c, enter, entering, *gates)


def normed_kernel(at_ref, g_ref, gain_ref, w_ref, first_ref, second_ref, normed_ref):
    quarters, rows, part = g_ref.shape

    @pl.when(pl.program_id(0) == 0)
    def _():
        squares = jnp.zeros((rows, part), F32)
        for q in range(quarters):
            g = g_ref[q].astype(F32)
            squares = squares + g * g
        squares = jnp.sum(squares, axis=1, keepdims=True)
        scale = lax.rsqrt(squares / (quarters * part) + EPS)
        for q in range(quarters):
            cols = slice(q * part, (q + 1) * part)
            normed_ref[:, cols] = (g_ref[q].astype(F32) * scale * gain_ref[:, cols]).astype(BF16)

    for side, o_ref in enumerate((first_ref, second_ref)):

        @pl.when(pl.program_id(0) == side)
        def _():
            o_ref[...] = dot(normed_ref[...], w_ref[...]).astype(BF16)


def out_kernel(at_ref, normed_ref, w_ref, o_ref):
    o_ref[0] = dot(normed_ref[...], w_ref[...]).astype(BF16)


def out_partial(at, targets, inputs, w, rows, width):
    count = len(targets)
    cores = 2
    places = w.shape[1] // (width * cores)

    def tile(i, t):
        distance, other = 0, 0
        for j, (d, o) in enumerate(targets):
            distance = jnp.where(i == j, d, distance)
            other = jnp.where(i == j, o, other)
        return lax.rem(t[0] + distance, places) * cores + jnp.where(other == 1, 1 - t[1], t[1])

    first = len(inputs) > 1
    keep = lambda a: pl.BlockSpec(a.shape, lambda i, t: (0,) * len(a.shape))
    normed = jax.ShapeDtypeStruct((rows, w.shape[0]), BF16)
    one = jax.ShapeDtypeStruct((rows, width), BF16)
    partial = jax.ShapeDtypeStruct((count, rows, width), BF16)
    partial_spec = pl.BlockSpec((1, rows, width), lambda i, t: (i, 0, 0))
    return pl.pallas_call(
        normed_kernel if first else out_kernel,
        grid_spec=pltpu.PrefetchScalarGridSpec(
            num_scalar_prefetch=1,
            grid=(count,),
            in_specs=[
                *(keep(a) for a in inputs),
                pl.BlockSpec((w.shape[0], width), lambda i, t: (0, tile(i, t))),
            ],
            out_specs=[keep(one), keep(one), keep(normed)] if first else partial_spec,
        ),
        out_shape=[one, one, normed] if first else partial,
        cost_estimate=cost(2 * w.shape[0] * rows * width * count, partial, normed),
        name="out_normed" if first else "out_partial",
    )(at, *inputs, w)


def out_shares(gated, gain, w, feats):
    rows = gated.shape[1]
    at = jnp.stack([lax.axis_index("y"), lax.axis_index("c")])
    far_other, far, normed = out_partial(
        at, ((2, 1), (2, 0)), (gated, gain), w, rows, feats
    )
    far_other = shifted(far_other, "c", 1)
    near_other = out_partial(at, ((1, 1), (3, 1), (0, 1)), (normed,), w, rows, feats)
    near_other = shifted(near_other, "c", 1)
    far = (far.astype(F32) + far_other.astype(F32)).astype(BF16)
    upper = shifted(far[: rows // 2], "y", 1)
    lower = shifted(far[rows // 2 :], "y", -1)
    near = out_partial(at, ((1, 0), (3, 0), (0, 0)), (normed,), w, rows, feats)
    blank = jnp.zeros((rows // 2, feats), F32)
    near = [n.astype(F32) + o.astype(F32) for n, o in zip(near, near_other)]
    up = near[0] + jnp.concatenate([upper.astype(F32), blank], axis=0)
    down = near[1] + jnp.concatenate([blank, lower.astype(F32)], axis=0)
    up, down = shifted(up.astype(BF16), "y", 1), shifted(down.astype(BF16), "y", -1)
    return near[2] + up.astype(F32) + down.astype(F32)


def gathered_weights(packed, low, edge):
    nz, zi = lax.axis_size("z"), lax.axis_index("z")
    half = nz // 2
    left = right = packed
    blocks, distances = [packed], [0]
    for step in range(1, half):
        left, right = shifted(left, "z", 1), shifted(right, "z", -1)
        if step == 1:
            left, right, edge = lax.optimization_barrier((left, right, edge))
        blocks += [left, right]
        distances += [-step, step]
    far_low = shifted(left[..., :low], "z", 1)
    far_gate = shifted(right[..., low:], "z", -1)
    place = lax.rem(zi + jnp.array([*distances, half], jnp.int32) + nz, nz)
    peers = lax.axis_size(("x", "y", "c"))
    edges = lax.all_to_all(
        jnp.broadcast_to(edge[None], (peers, *edge.shape)), ("x", "y", "c"), 0, 0, tiled=True
    )
    return place, (*blocks, far_low), (*blocks, far_gate), edges


def local(
    hidden_in,
    norm_gain,
    w_x,
    w_z,
    w_bc,
    w_dt,
    dt_bias,
    decay_rate,
    conv_x,
    conv_bc,
    conv_bias_x,
    conv_bias_bc,
    skip_d,
    out_gain,
    w_out,
):
    nx, nz, ny, nc = (lax.axis_size(a) for a in ("x", "z", "y", "c"))
    xi, zi = (lax.axis_index(a) for a in ("x", "z"))
    rows, feats = hidden_in.shape
    depth, width = w_x.shape
    part = width // nx
    bc_width = w_bc.shape[2]
    bc_part = bc_width // nx
    heads = decay_rate.shape[0]
    own_heads = heads // nx
    taps = conv_x.shape[0]
    low = -(-(part + bc_part + own_heads) // 128) * 128
    spare = low - part - bc_part - own_heads

    gathered = lax.all_gather(hidden_in, ("x", "y", "c"), axis=0)
    gathered = gathered.reshape(nx, ny * nc, rows, feats)
    route = [(i, i + 1) for i in range(nx * nz - 1)]
    edge = lax.ppermute(hidden_in[rows - LEAD :], ("x", "z"), route)

    gain = lax.dynamic_slice(norm_gain, ((xi * nz + zi) * depth,), (depth,))
    pieces = [w.reshape(depth, nx, -1) for w in (w_x, w_bc, w_dt)]
    pieces.append(jnp.zeros((depth, nx, spare), BF16))
    pieces.append(w_z.reshape(depth, nx, part))
    packed = jnp.concatenate(pieces, axis=2).astype(F32) * gain[:, None, None]
    packed = jnp.transpose(packed.astype(BF16), (1, 0, 2))
    packed = lax.all_to_all(packed, "x", 0, 0, tiled=True)
    place, w_low, w_gate, edges = lax.optimization_barrier(gathered_weights(packed, low, edge))
    edges = edges.reshape(nx, ny * nc, LEAD, feats)

    def own(a):
        size = a.shape[-1] // nx
        return lax.dynamic_slice_in_dim(a, xi * size, size, axis=a.ndim - 1)

    row = lambda a: a.reshape(1, -1)
    tap_rows = jnp.concatenate([own(conv_x), own(conv_bc.reshape(taps, -1))], axis=1)
    tap_rows = jnp.pad(tap_rows, ((0, 0), (0, own_heads + spare)))
    bias_row = jnp.concatenate([own(conv_bias_x), own(conv_bias_bc.reshape(-1))])
    bias_row = row(jnp.pad(bias_row, (0, own_heads + spare)))
    in_lanes = lambda a: row(jnp.pad(own(a), (bc_part, spare)))
    x_conv, quarter, dt = project(
        place, edges, gathered, w_low, tap_rows, bias_row, in_lanes(dt_bias), part, bc_part
    )
    head = width // heads
    half = nx // 2
    quarters, (cum, scaled), early_gate = lax.optimization_barrier(
        (
            lax.all_to_all(quarter, "x", 0, 0, tiled=True),
            block_decays(x_conv, dt, in_lanes(decay_rate), bc_part, head),
            project_gate(place, gathered, w_gate, dt, low, 0, half),
        )
    )
    skip_row = row(jnp.repeat(own(skip_d), head))
    enter, message = block_states(scaled, quarters, cum, bc_part, head, nz)
    received, (y, c_rows) = lax.optimization_barrier(
        (
            lax.all_to_all(message, "z", 0, 0, tiled=True),
            intra_blocks(x_conv, quarters, dt, cum, skip_row, bc_part, head),
        )
    )
    states = combine_states(received, nx)
    states, gate_inputs = lax.optimization_barrier((states, gathered))
    entering, late_gate = lax.optimization_barrier(
        (
            lax.all_to_all(states, "z", 0, 0, tiled=True),
            project_gate(place, gate_inputs, w_gate, dt, low, half, nx - half),
        )
    )
    gates = (early_gate, late_gate)
    gated = gate_blocks(y, cum, c_rows, enter, entering, gates, bc_part, head)
    gated = lax.all_to_all(gated, "x", 0, 0, tiled=True)

    summed = out_shares(gated, row(out_gain), w_out, feats)
    return (hidden_in.astype(F32) + summed).astype(BF16)


def solution(mesh):
    sizes = mesh.shape
    devices = mesh.devices.reshape(4, sizes["seq"] // 4, sizes["tensor"] // 2, 2)
    split = Mesh(devices, ("x", "z", "y", "c"))
    seq, tensor = ("x", "z"), ("y", "c")
    in_specs = (
        P(seq, tensor),
        P(),
        P(seq, tensor),
        P(seq, tensor),
        P(seq, tensor, None),
        P(seq, tensor),
        P(tensor),
        P(tensor),
        P(None, tensor),
        P(None, tensor, None),
        P(tensor),
        P(tensor, None),
        P(tensor),
        P(tensor),
        P(tensor, None),
    )
    return jax.shard_map(
        local, mesh=split, in_specs=in_specs, out_specs=P(seq, tensor), check_vma=False
    )
```

```python
import functools

import jax
import jax.numpy as jnp
from jax import lax
from jax.experimental import pallas as pl
from jax.experimental.pallas import tpu as pltpu
from jax.sharding import Mesh
from jax.sharding import PartitionSpec as P

SPAN = 128
LEAD = 16
EPS = 1e-05
F32, BF16 = jnp.float32, jnp.bfloat16


def dot(a, b):
    return jnp.dot(a, b, preferred_element_type=F32)


def shifted(block, axis, distance):
    n = lax.axis_size(axis)
    return lax.ppermute(block, axis, [(i, (i + distance) % n) for i in range(n)])


def silu(v):
    return v * jax.nn.sigmoid(v)


def whole(a):
    return pl.BlockSpec(a.shape, lambda s: (0,) * a.ndim)


def each(a):
    return pl.BlockSpec((1, *a.shape[1:]), lambda s: (s,) + (0,) * (a.ndim - 1))


def cost(flops, *arrays):
    moved = sum(a.size * a.dtype.itemsize for a in arrays)
    return pl.CostEstimate(flops=flops, bytes_accessed=moved, transcendentals=0)


def block_copies(blocks, lanes, place_ref, w, sems):
    segments, depth = blocks[0].shape[:2]
    copies = []
    for b, block in enumerate(blocks):
        low = min(lanes, block.shape[2] - w.shape[1])
        for s in range(segments):
            row = pl.multiple_of((s * len(blocks) + place_ref[b]) * depth, depth)
            copies.append(
                pltpu.make_async_copy(
                    block.at[s, :, pl.ds(low, w.shape[1])],
                    w.at[pl.ds(row, depth), :],
                    sems.at[b, s],
                )
            )
    return copies


def proj_kernel(halves, count, place_ref, edge_ref, h_ref, *refs):
    blocks, refs = refs[:count], refs[count:]
    taps_ref, bias_ref, dt_bias_ref, x_ref, bc_ref, dt_ref, w_ref, acc, pre, sems = refs

    @pl.when(pl.program_id(0) == 0)
    def _():
        copies = block_copies(blocks, 0, place_ref, w_ref, sems)
        for copy in copies:
            copy.start()
        for copy in copies:
            copy.wait()

    pieces, feats = h_ref.shape[1], h_ref.shape[3]
    part, total = x_ref.shape[2], pieces * feats
    rows, bc_part = x_ref.shape[1], bc_ref.shape[3] // halves
    lanes = min(128, feats)
    step = pieces // 2
    squares = None
    for j in range(0, pieces, step):
        tall = []
        for i in range(j, j + step):
            h = jnp.concatenate([edge_ref[0, i], h_ref[0, i]], axis=0)
            tall.append(h)
            wide = h.astype(F32)
            for k in range(0, feats, lanes):
                square = wide[:, k : k + lanes] * wide[:, k : k + lanes]
                squares = square if squares is None else squares + square
        product = dot(jnp.concatenate(tall, axis=1), w_ref[j * feats : (j + step) * feats, :])
        if j == 0:
            acc[...] = product
        else:
            acc[...] += product
    scale = lax.rsqrt(jnp.sum(squares, axis=1, keepdims=True) / total + EPS)
    spare = dt_ref.shape[2]
    dt_raw = acc[LEAD:, part:] * scale[LEAD:] + dt_bias_ref[...]
    dt = jnp.maximum(dt_raw, 0.0) + jnp.log1p(jnp.exp(-jnp.abs(dt_raw)))
    lane = lax.broadcasted_iota(jnp.int32, dt.shape, 1)
    dt_ref[0] = jnp.where(lane == spare - 1, scale[LEAD:], dt)
    pre[...] = (acc[...] * scale).astype(BF16).astype(F32)
    taps = taps_ref.shape[0]
    running = bias_ref[...]
    for k in range(taps):
        start = LEAD - taps + 1 + k
        running = running + taps_ref[k : k + 1] * pre[start : start + rows]
    mixed = silu(running).astype(BF16)
    x_ref[0] = mixed[:, :part]
    quarter = mixed[:, part : part + bc_part]
    for side in range(halves):

        @pl.when(lax.rem(pl.program_id(0), halves) == side)
        def _():
            for q in range(bc_ref.shape[0]):
                bc_ref[q, 0, :, side * bc_part : (side + 1) * bc_part] = quarter


def project(place, edge, h, blocks, taps, bias, dt_bias, part, bc_part):
    segments, pieces, rows, feats = h.shape
    low, total = taps.shape[1], pieces * feats
    out = lambda width: pl.BlockSpec((1, rows, width), lambda s, p: (s, 0, 0))
    shape = lambda width, dtype: jax.ShapeDtypeStruct((segments, rows, width), dtype)
    keep = lambda a: pl.BlockSpec(a.shape, lambda s, p: (0,) * a.ndim)
    step = lambda a: pl.BlockSpec((1, *a.shape[1:]), lambda s, p: (s, 0, 0, 0))
    packed = (segments, segments // 2, rows, 2 * bc_part)
    return pl.pallas_call(
        functools.partial(proj_kernel, 2, len(blocks)),
        grid_spec=pltpu.PrefetchScalarGridSpec(
            num_scalar_prefetch=1,
            grid=(segments,),
            in_specs=[
                step(edge),
                step(h),
                *(pl.BlockSpec(memory_space=pl.ANY) for _ in blocks),
                keep(taps),
                keep(bias),
                keep(dt_bias),
            ],
            out_specs=[
                out(part),
                pl.BlockSpec((segments, 1, *packed[2:]), lambda s, p: (0, s // 2, 0, 0)),
                out(low - part),
            ],
            scratch_shapes=[
                pltpu.VMEM((total, low), BF16),
                pltpu.VMEM((rows + LEAD, low), F32),
                pltpu.VMEM((rows + LEAD, low), F32),
                pltpu.SemaphoreType.DMA((len(blocks), segments)),
            ],
        ),
        out_shape=[
            shape(part, BF16),
            jax.ShapeDtypeStruct(packed, BF16),
            shape(low - part, F32),
        ],
        cost_estimate=cost(2 * h.size * low, h),
        name="project",
    )(place, edge, h, *blocks, taps, bias, dt_bias)


def gate_proj_kernel(count, low, place_ref, h_ref, *refs):
    blocks, (dt_ref, z_ref, w_ref, sems) = refs[:count], refs[count:]

    @pl.when(pl.program_id(0) == 0)
    def _():
        copies = block_copies(blocks, low, place_ref, w_ref, sems)
        for copy in copies:
            copy.start()
        for copy in copies:
            copy.wait()

    pieces = h_ref.shape[1]
    tall = jnp.concatenate([h_ref[0, j] for j in range(pieces)], axis=1)
    scale = dt_ref[0, :, dt_ref.shape[2] - 1 :]
    z_ref[0] = (dot(tall, w_ref[...]) * scale).astype(BF16)


def project_gate(place, h, blocks, dt, low, start, count):
    pieces, rows, feats = h.shape[1:]
    part = blocks[0].shape[2] - low
    return pl.pallas_call(
        functools.partial(gate_proj_kernel, len(blocks), low),
        grid_spec=pltpu.PrefetchScalarGridSpec(
            num_scalar_prefetch=1,
            grid=(count,),
            in_specs=[
                pl.BlockSpec((1, pieces, rows, feats), lambda s, p: (s + start, 0, 0, 0)),
                *(pl.BlockSpec(memory_space=pl.ANY) for _ in blocks),
                pl.BlockSpec((1, *dt.shape[1:]), lambda s, p: (s + start, 0, 0)),
            ],
            out_specs=pl.BlockSpec((1, rows, part), lambda s, p: (s, 0, 0)),
            scratch_shapes=[
                pltpu.VMEM((pieces * feats, part), BF16),
                pltpu.SemaphoreType.DMA((len(blocks), blocks[0].shape[0])),
            ],
        ),
        out_shape=jax.ShapeDtypeStruct((count, rows, part), BF16),
        cost_estimate=cost(2 * h.size * part * count // h.shape[0], h),
        name="project_gate",
    )(place, h, *blocks, dt)


def group_rows(quarters_ref, at, first):
    count, width = quarters_ref.shape[0] // 2, quarters_ref.shape[3] // 2
    odd = lax.rem(pl.program_id(0), 2) == 1
    parts = []
    for q in range(count):
        pair = quarters_ref[first * count + q, 0, at]
        parts.append(jnp.where(odd, pair[:, width:], pair[:, :width]))
    return jnp.concatenate(parts, axis=1)


def lower_mask():
    pick = lambda axis: lax.broadcasted_iota(jnp.int32, (SPAN, SPAN), axis)
    return pick(0) >= pick(1)


def decay_kernel(first, head, x_ref, dt_ref, rate_ref, cum_ref, scaled_ref):
    rows, part = x_ref.shape[1:]
    lower = lower_mask().astype(F32)
    for b in range(rows // SPAN):
        at = slice(b * SPAN, (b + 1) * SPAN)
        dt = dt_ref[0, at]
        cum = jnp.dot(
            lower, -dt * rate_ref[...], precision=lax.Precision.HIGHEST, preferred_element_type=F32
        )
        cum_ref[0, at] = cum
        tail = jnp.exp(cum[SPAN - 1 : SPAN] - cum) * dt
        for h in range(part // head):
            cols = slice(h * head, (h + 1) * head)
            wide = x_ref[0, at, cols].astype(F32)
            scaled_ref[0, at, cols] = (wide * tail[:, first + h : first + h + 1]).astype(BF16)


def block_decays(x, dt, rate, first, head):
    return pl.pallas_call(
        functools.partial(decay_kernel, first, head),
        grid=(x.shape[0],),
        in_specs=[each(x), each(dt), whole(rate)],
        out_specs=[each(dt), each(x)],
        out_shape=[
            jax.ShapeDtypeStruct(dt.shape, F32),
            jax.ShapeDtypeStruct(x.shape, BF16),
        ],
        cost_estimate=cost(16 * dt.size * SPAN, x, x, dt, dt),
        name="block_decays",
    )(x, dt, rate)


def states_kernel(first, head, scaled_ref, quarters_ref, cum_ref, enter_ref, message_ref, logs):
    rows, part = scaled_ref.shape[1:]
    segments, chunks = pl.num_programs(0), message_ref.shape[0]
    s = pl.program_id(0)
    base = jnp.zeros_like(cum_ref[0, :1])
    state = None
    for b in range(rows // SPAN):
        at = slice(b * SPAN, (b + 1) * SPAN)
        last = cum_ref[0, (b + 1) * SPAN - 1 : (b + 1) * SPAN]
        base = base + last
        fresh = dot(group_rows(quarters_ref, at, 0).T, scaled_ref[0, at])
        if b:
            enter_ref[0, b - 1] = state
            decay = [
                jnp.broadcast_to(jnp.exp(last[:, first + h : first + h + 1]), (1, head))
                for h in range(part // head)
            ]
            fresh = jnp.concatenate(decay, axis=1) * state + fresh
        state = fresh
    deep = state.shape[0] // chunks
    place = pl.ds(pl.multiple_of(s * deep, deep), deep)
    message_ref[:, place, :] = state.reshape(chunks, deep, part).astype(BF16)
    for h in range(part // head):
        cols = slice(h * head, (h + 1) * head)
        log = jnp.broadcast_to(base[:, first + h : first + h + 1], (1, head))
        high = log.astype(BF16).astype(F32)
        row = lax.broadcasted_iota(jnp.int32, (logs.shape[0], head), 0)
        kept = jnp.where(row == 2 * s + 1, log - high, logs[:, cols])
        logs[:, cols] = jnp.where(row == 2 * s, high, kept)

    @pl.when(s == segments - 1)
    def _():
        tail_rows = logs[...].astype(BF16)
        for q in range(chunks):
            message_ref[q, message_ref.shape[1] - logs.shape[0] :, :] = tail_rows


def quarters_spec(quarters):
    return pl.BlockSpec((quarters.shape[0], 1, *quarters.shape[2:]), lambda s: (0, s // 2, 0, 0))


def block_states(scaled, quarters, cum, first, head, chunks):
    segments, rows, part = scaled.shape
    n = quarters.shape[0] // 2 * quarters.shape[3] // 2
    message = (chunks, segments * n // chunks + 2 * segments, part)
    enter = jax.ShapeDtypeStruct((segments, rows // SPAN - 1, n, part), F32)
    return pl.pallas_call(
        functools.partial(states_kernel, first, head),
        grid=(segments,),
        in_specs=[each(scaled), quarters_spec(quarters), each(cum)],
        out_specs=[each(enter), pl.BlockSpec(message, lambda s: (0, 0, 0))],
        out_shape=[enter, jax.ShapeDtypeStruct(message, BF16)],
        scratch_shapes=[pltpu.VMEM((2 * segments, part), F32)],
        cost_estimate=cost(2 * scaled.size * n, scaled, cum, enter),
        name="block_states",
    )(scaled, quarters, cum)


def intra_kernel(first, head, x_ref, quarters_ref, dt_ref, cum_ref, skip_ref, y_ref, c_ref):
    rows, part = x_ref.shape[1:]
    mask = lower_mask()
    for b in range(rows // SPAN):
        at = slice(b * SPAN, (b + 1) * SPAN)
        cum = cum_ref[0, at]
        cum_rows, dt_rows = cum.T, dt_ref[0, at].T
        c_block = group_rows(quarters_ref, at, 1)
        c_ref[0, at] = c_block
        scores = lax.dot_general(
            c_block,
            group_rows(quarters_ref, at, 0),
            (((1,), (1,)), ((), ())),
            preferred_element_type=F32,
        )
        for h in range(part // head):
            lane = slice(first + h, first + h + 1)
            cols = slice(h * head, (h + 1) * head)
            gap = cum[:, lane] - cum_rows[lane]
            decay = jnp.where(mask, jnp.exp(jnp.where(mask, gap, 0.0)), 0.0)
            mix = (scores * decay * dt_rows[lane]).astype(BF16)
            x = x_ref[0, at, cols]
            y_ref[0, at, cols] = dot(mix, x) + skip_ref[:, cols] * x.astype(F32)


def intra_blocks(x, quarters, dt, cum, skip, first, head):
    segments, rows, _ = x.shape
    n = quarters.shape[0] // 2 * quarters.shape[3] // 2
    return pl.pallas_call(
        functools.partial(intra_kernel, first, head),
        grid=(segments,),
        in_specs=[each(x), quarters_spec(quarters), each(dt), each(cum), whole(skip)],
        out_specs=[each(x), pl.BlockSpec((1, rows, n), lambda s: (s, 0, 0))],
        out_shape=[
            jax.ShapeDtypeStruct(x.shape, F32),
            jax.ShapeDtypeStruct((segments, rows, n), BF16),
        ],
        cost_estimate=cost(64 * x.size * SPAN, x, x, x, dt, cum),
        name="intra_blocks",
    )(x, quarters, dt, cum, skip)


def combine_kernel(segments, r_ref, o_ref):
    places, part = r_ref.shape[0], r_ref.shape[2]
    deep = o_ref.shape[1] // segments
    logs = r_ref[:, segments * deep :, :].astype(F32)
    state = jnp.zeros((deep, part), F32)
    for s in range(segments):
        at = slice(s * deep, (s + 1) * deep)
        for z in range(places):
            o_ref[z, at] = state.astype(BF16)
            decay = jnp.exp(logs[z, 2 * s : 2 * s + 1] + logs[z, 2 * s + 1 : 2 * s + 2])
            state = decay * state + r_ref[z, at].astype(F32)


def combine_states(received, segments):
    places, deep, part = received.shape
    return pl.pallas_call(
        functools.partial(combine_kernel, segments),
        out_shape=jax.ShapeDtypeStruct((places, deep - 2 * segments, part), BF16),
        name="combine_states",
    )(received)


def gate_kernel(first, head, half, y_ref, cum_ref, c_ref, enter_ref, s_ref, z0_ref, z1_ref, o_ref):
    rows, part = y_ref.shape[1:]
    incoming = s_ref[...].reshape(c_ref.shape[2], part).astype(F32)
    base = jnp.zeros_like(cum_ref[0, :1])
    for b in range(rows // SPAN):
        at = slice(b * SPAN, (b + 1) * SPAN)
        cum = cum_ref[0, at]
        for h in range(part // head):
            lane = slice(first + h, first + h + 1)
            cols = slice(h * head, (h + 1) * head)
            enter = incoming[:, cols]
            if b:
                enter = jnp.exp(base[:, lane]) * enter + enter_ref[0, b - 1, :, cols]
            inter = dot(c_ref[0, at], enter.astype(BF16))
            y = y_ref[0, at, cols] + jnp.exp(cum[:, lane]) * inter
            early = pl.program_id(0) < half
            z = jnp.where(early, z0_ref[0, at, cols], z1_ref[0, at, cols]).astype(F32)
            o_ref[0, at, cols] = (y * silu(z)).astype(BF16)
        base = base + cum[SPAN - 1 :]


def gate_blocks(y, cum, c, enter, entering, gates, first, head):
    segments, rows, part = y.shape
    deep = entering.shape[1] // segments
    half = gates[0].shape[0]
    out = jax.ShapeDtypeStruct(y.shape, BF16)
    return pl.pallas_call(
        functools.partial(gate_kernel, first, head, half),
        grid=(segments,),
        in_specs=[
            each(y),
            each(cum),
            each(c),
            each(enter),
            pl.BlockSpec((entering.shape[0], deep, part), lambda s: (0, s, 0)),
            pl.BlockSpec((1, rows, part), lambda s: (jnp.minimum(s, half - 1), 0, 0)),
            pl.BlockSpec((1, rows, part), lambda s: (jnp.maximum(s - half, 0), 0, 0)),
        ],
        out_specs=each(out),
        out_shape=out,
        cost_estimate=cost(2 * y.size * c.shape[2], y, cum, c, enter, out, out),
        name="gate_blocks",
    )(y, cum, c, enter, entering, *gates)


def normed_kernel(at_ref, g_ref, gain_ref, w_ref, first_ref, second_ref, normed_ref):
    quarters, rows, part = g_ref.shape

    @pl.when(pl.program_id(0) == 0)
    def _():
        squares = jnp.zeros((rows, part), F32)
        for q in range(quarters):
            g = g_ref[q].astype(F32)
            squares = squares + g * g
        squares = jnp.sum(squares, axis=1, keepdims=True)
        scale = lax.rsqrt(squares / (quarters * part) + EPS)
        for q in range(quarters):
            cols = slice(q * part, (q + 1) * part)
            normed_ref[:, cols] = (g_ref[q].astype(F32) * scale * gain_ref[:, cols]).astype(BF16)

    for side, o_ref in enumerate((first_ref, second_ref)):

        @pl.when(pl.program_id(0) == side)
        def _():
            o_ref[...] = dot(normed_ref[...], w_ref[...]).astype(BF16)


def out_kernel(at_ref, normed_ref, w_ref, o_ref):
    o_ref[0] = dot(normed_ref[...], w_ref[...]).astype(BF16)


def out_partial(at, targets, inputs, w, rows, width):
    count = len(targets)
    cores = 2
    places = w.shape[1] // (width * cores)

    def tile(i, t):
        distance, other = 0, 0
        for j, (d, o) in enumerate(targets):
            distance = jnp.where(i == j, d, distance)
            other = jnp.where(i == j, o, other)
        return lax.rem(t[0] + distance, places) * cores + jnp.where(other == 1, 1 - t[1], t[1])

    first = len(inputs) > 1
    keep = lambda a: pl.BlockSpec(a.shape, lambda i, t: (0,) * len(a.shape))
    normed = jax.ShapeDtypeStruct((rows, w.shape[0]), BF16)
    one = jax.ShapeDtypeStruct((rows, width), BF16)
    partial = jax.ShapeDtypeStruct((count, rows, width), BF16)
    partial_spec = pl.BlockSpec((1, rows, width), lambda i, t: (i, 0, 0))
    return pl.pallas_call(
        normed_kernel if first else out_kernel,
        grid_spec=pltpu.PrefetchScalarGridSpec(
            num_scalar_prefetch=1,
            grid=(count,),
            in_specs=[
                *(keep(a) for a in inputs),
                pl.BlockSpec((w.shape[0], width), lambda i, t: (0, tile(i, t))),
            ],
            out_specs=[keep(one), keep(one), keep(normed)] if first else partial_spec,
        ),
        out_shape=[one, one, normed] if first else partial,
        cost_estimate=cost(2 * w.shape[0] * rows * width * count, partial, normed),
        name="out_normed" if first else "out_partial",
    )(at, *inputs, w)


def out_shares(at, gated, gain, w, feats):
    rows = gated.shape[1]
    far_other, far, normed = out_partial(
        at, ((2, 1), (2, 0)), (gated, gain), w, rows, feats
    )
    far_other = shifted(far_other, "c", 1)
    near_other = out_partial(at, ((1, 1), (3, 1), (0, 1)), (normed,), w, rows, feats)
    near_other = shifted(near_other, "c", 1)
    far = (far.astype(F32) + far_other.astype(F32)).astype(BF16)
    upper = shifted(far[: rows // 2], "y", 1)
    lower = shifted(far[rows // 2 :], "y", -1)
    near = out_partial(at, ((1, 0), (3, 0), (0, 0)), (normed,), w, rows, feats)
    blank = jnp.zeros((rows // 2, feats), F32)
    near = [n.astype(F32) + o.astype(F32) for n, o in zip(near, near_other)]
    up = near[0] + jnp.concatenate([upper.astype(F32), blank], axis=0)
    down = near[1] + jnp.concatenate([blank, lower.astype(F32)], axis=0)
    up, down = shifted(up.astype(BF16), "y", 1), shifted(down.astype(BF16), "y", -1)
    return near[2] + up.astype(F32) + down.astype(F32)


def gathered_weights(packed, low, edge):
    nz, zi = lax.axis_size("z"), lax.axis_index("z")
    half = nz // 2
    left = right = packed
    blocks, distances = [packed], [0]
    for step in range(1, half):
        left, right = shifted(left, "z", 1), shifted(right, "z", -1)
        if step == 1:
            left, right, edge = lax.optimization_barrier((left, right, edge))
        blocks += [left, right]
        distances += [-step, step]
    far_low = shifted(left[..., :low], "z", 1)
    far_gate = shifted(right[..., low:], "z", -1)
    place = lax.rem(zi + jnp.array([*distances, half], jnp.int32) + nz, nz)
    peers = lax.axis_size(("x", "y", "c"))
    edges = lax.all_to_all(
        jnp.broadcast_to(edge[None], (peers, *edge.shape)), ("x", "y", "c"), 0, 0, tiled=True
    )
    return place, (*blocks, far_low), (*blocks, far_gate), edges


def local(
    hidden_in,
    norm_gain,
    w_x,
    w_z,
    w_bc,
    w_dt,
    dt_bias,
    decay_rate,
    conv_x,
    conv_bc,
    conv_bias_x,
    conv_bias_bc,
    skip_d,
    out_gain,
    w_out,
):
    nx, nz, ny, nc = (lax.axis_size(a) for a in ("x", "z", "y", "c"))
    xi, zi = (lax.axis_index(a) for a in ("x", "z"))
    rows, feats = hidden_in.shape
    depth, width = w_x.shape
    part = width // nx
    bc_width = w_bc.shape[2]
    bc_part = bc_width // nx
    heads = decay_rate.shape[0]
    own_heads = heads // nx
    taps = conv_x.shape[0]
    low = -(-(part + bc_part + own_heads) // 128) * 128
    spare = low - part - bc_part - own_heads

    gathered = lax.all_gather(hidden_in, ("x", "y", "c"), axis=0)
    gathered = gathered.reshape(nx, ny * nc, rows, feats)
    route = [(i, i + 1) for i in range(nx * nz - 1)]
    edge = lax.ppermute(hidden_in[rows - LEAD :], ("x", "z"), route)

    gain = lax.dynamic_slice(norm_gain, ((xi * nz + zi) * depth,), (depth,))
    pieces = [w.reshape(depth, nx, -1) for w in (w_x, w_bc, w_dt)]
    pieces.append(jnp.zeros((depth, nx, spare), BF16))
    pieces.append(w_z.reshape(depth, nx, part))
    packed = jnp.concatenate(pieces, axis=2).astype(F32) * gain[:, None, None]
    packed = jnp.transpose(packed.astype(BF16), (1, 0, 2))
    packed = lax.all_to_all(packed, "x", 0, 0, tiled=True)
    ring = gathered_weights(packed, low, edge)

    def own(a):
        size = a.shape[-1] // nx
        return lax.dynamic_slice_in_dim(a, xi * size, size, axis=a.ndim - 1)

    row = lambda a: a.reshape(1, -1)
    tap_rows = jnp.concatenate([own(conv_x), own(conv_bc.reshape(taps, -1))], axis=1)
    tap_rows = jnp.pad(tap_rows, ((0, 0), (0, own_heads + spare)))
    bias_row = jnp.concatenate([own(conv_bias_x), own(conv_bias_bc.reshape(-1))])
    bias_row = row(jnp.pad(bias_row, (0, own_heads + spare)))
    in_lanes = lambda a: row(jnp.pad(own(a), (bc_part, spare)))
    head = width // heads
    rows_of = (
        in_lanes(dt_bias),
        in_lanes(decay_rate),
        row(jnp.repeat(own(skip_d), head)),
        jnp.stack([lax.axis_index("y"), lax.axis_index("c")]),
    )
    ring, rows_of = lax.optimization_barrier((ring, rows_of))
    place, w_low, w_gate, edges = ring
    dt_bias_row, rate_row, skip_row, at = rows_of
    edges = edges.reshape(nx, ny * nc, LEAD, feats)
    x_conv, quarter, dt = project(
        place, edges, gathered, w_low, tap_rows, bias_row, dt_bias_row, part, bc_part
    )
    half = nx // 2
    quarters, (cum, scaled), early_gate = lax.optimization_barrier(
        (
            lax.all_to_all(quarter, "x", 0, 0, tiled=True),
            block_decays(x_conv, dt, rate_row, bc_part, head),
            project_gate(place, gathered, w_gate, dt, low, 0, half),
        )
    )
    enter, message = block_states(scaled, quarters, cum, bc_part, head, nz)
    received, (y, c_rows) = lax.optimization_barrier(
        (
            lax.all_to_all(message, "z", 0, 0, tiled=True),
            intra_blocks(x_conv, quarters, dt, cum, skip_row, bc_part, head),
        )
    )
    states = combine_states(received, nx)
    states, gate_inputs = lax.optimization_barrier((states, gathered))
    entering, late_gate = lax.optimization_barrier(
        (
            lax.all_to_all(states, "z", 0, 0, tiled=True),
            project_gate(place, gate_inputs, w_gate, dt, low, half, nx - half),
        )
    )
    gates = (early_gate, late_gate)
    gated = gate_blocks(y, cum, c_rows, enter, entering, gates, bc_part, head)
    gated = lax.all_to_all(gated, "x", 0, 0, tiled=True)

    summed = out_shares(at, gated, row(out_gain), w_out, feats)
    return (hidden_in.astype(F32) + summed).astype(BF16)


def solution(mesh):
    sizes = mesh.shape
    devices = mesh.devices.reshape(4, sizes["seq"] // 4, sizes["tensor"] // 2, 2)
    split = Mesh(devices, ("x", "z", "y", "c"))
    seq, tensor = ("x", "z"), ("y", "c")
    in_specs = (
        P(seq, tensor),
        P(),
        P(seq, tensor),
        P(seq, tensor),
        P(seq, tensor, None),
        P(seq, tensor),
        P(tensor),
        P(tensor),
        P(None, tensor),
        P(None, tensor, None),
        P(tensor),
        P(tensor, None),
        P(tensor),
        P(tensor),
        P(tensor, None),
    )
    return jax.shard_map(
        local, mesh=split, in_specs=in_specs, out_specs=P(seq, tensor), check_vma=False
    )
```
